32 devices in a mesh: ctx: 4 (over y, x), head: 4 (over z), rep: 2 (over core).
Axes of the slice: x: 2, y: 2, z: 4, core: 2. Of those that a mesh axis runs over, the one named last changes fastest.
Arguments:
- queries: bfloat16 [512, 3072], P(('rep', 'ctx'), 'head'), parts along dimension 0, may hold values from -18 to 18
- kv_latent: bfloat16 [512, 576], P(('rep', 'ctx')), parts along dimension 0, may hold values from -140 to 140
- doc_ids: int32 [512], P(('rep', 'ctx')), parts along dimension 0, may hold values from 0 to 3, never falling along the last dimension, each value on 1 to 128 neighbouring positions
- w_kv: bfloat16 [512, 4096], P(None, 'head'), may hold values from -0.25 to 0.25
- w_out: bfloat16 [2048, 7168], P('head'), may hold values from -0.5 to 0.5
- w_enc: bfloat16 [7168, 576], P('head'), may hold values from -0.0625 to 0.0625
- residual: bfloat16 [512, 7168], P(('rep', 'ctx'), 'head'), parts along dimension 0, may hold values from -32 to 32
- norm_gain: float32 [7168], P('head'), may hold values from 0.1 to 1.9
Outputs:
- attn_out: bfloat16 [512, 7168], P(('rep', 'ctx'), 'head'), parts along dimension 0
- next_latent: bfloat16 [512, 576], P(('rep', 'ctx')), parts along dimension 0
The draws below stay inside these ranges and needn't reach their ends.
There are 2 independent parts, one for each index of `rep`. The reference program is written for one: setup_inputs(seed, part) draws one part's arguments, and reference() takes and returns one part's arrays. A program takes and returns all parts, laid end to end along the dimension named above; an argument that names none is the same for every part. Nothing has to cross between parts.
Inputs may be any that keep to these rules, and one draw needn't show every extreme that they name: `doc_ids`: never falls along the window; every document number of 0 to 3 occurs, a document spans 1 to 128 tokens and one spans exactly 128.
All inputs are finite; a program needn't handle non-finite values.
Results may differ from the reference program's by a relative error of at most 0.0082.
Values may be sent and summed in bfloat16 or wider, within the bound.
A program may use at most 64 MiB of HBM per device.

```python
import math
import jax
import jax.numpy as jnp
import numpy as np
from jax import lax

D = 7168
KVL = 512
ROPE = 64
NOPE = 128
VDIM = 128
DOCS = 4
TOKENS = 256
HEADS = 16


def draw_kv_latent(key, part):
    key_base = jax.random.fold_in(key, 11)
    return jnp.clip(jax.random.normal(key_base, (TOKENS, KVL + ROPE), jnp.float32), -6.0, 6.0).astype(jnp.bfloat16)


def draw_residual(key, part):
    key_base = jax.random.fold_in(key, 21)
    columns = jnp.arange(D, dtype=jnp.float32) / (D - 1)
    col_scale = 0.6 * jnp.exp(columns * jnp.log(3.0))
    base = jnp.clip(jax.random.normal(key_base, (TOKENS, D), jnp.float32), -6.0, 6.0)
    return (base * col_scale[None, :]).astype(jnp.bfloat16)


def level_of(rng, extent, cuts, least, largest):
    level, own = 1.0, jax.random.fold_in(rng, 6)
    for dim, blocks in cuts:
        heights = jnp.exp(jax.random.uniform(jax.random.fold_in(own, dim), (blocks,), jnp.float32, least / len(cuts), largest / len(cuts)))
        level = level * jnp.repeat(heights, extent[dim] // blocks).reshape([-1 if axis == dim else 1 for axis in range(len(extent))])
    return level


def profile(count, total, most, slope):
    portions = [(1 << 20) // math.isqrt(standing ** slope) + 1 for standing in range(2, count + 1)]
    rest, holding = total - most - (count - 1), [1] * (count - 1)
    while rest > 0:
        candidates = [i for i in range(count - 1) if holding[i] < most]
        whole, budget = sum([portions[i] for i in candidates]), rest
        for i in candidates:
            extra = min(most - holding[i], max(1, budget * portions[i] // whole), rest)
            holding[i] = holding[i] + extra
            rest = rest - extra
    return np.array([most] + holding)


def ragged(own_key, amount, total, bound, lean):
    if amount == 2:
        one = jax.random.randint(own_key, (), max(1, total - bound), min(bound, total - 1) + 1)
        return jnp.stack([one, total - one])
    tallies = jnp.asarray(profile(amount, total, bound, lean), jnp.int32)
    pairs = (amount - 1) // 2
    source_of, taker = tallies[1:1 + 2 * pairs:2], tallies[2:2 + 2 * pairs:2]
    room = jnp.minimum(source_of - 1, bound - taker)
    moved = jax.random.randint(jax.random.fold_in(own_key, 1), (pairs,), 0, 1 << 20) % (room + 1)
    tallies = tallies.at[1:1 + 2 * pairs:2].set(source_of - moved).at[2:2 + 2 * pairs:2].set(taker + moved)
    return tallies[jax.random.permutation(jax.random.fold_in(own_key, 2), amount)]


def bell_draw(key, extent, scale, reach, cuts=(), held_as=jnp.bfloat16):
    array = scale * jax.random.normal(key, extent, jnp.float32)
    if cuts:
        array = array * level_of(key, extent, cuts, -0.22, 0.18)
    return jnp.clip(array, -reach, reach).astype(held_as)


def setup_inputs(seed: int = 0, part: int = 0) -> dict:
    seeds = jax.random.split(jax.random.key(seed), 9)
    own_keys = jax.random.split(jax.random.fold_in(seeds[8], part), 9)
    queries = bell_draw(own_keys[0], (TOKENS, HEADS * (NOPE + ROPE)), 3.0, 18.0, ((0, 4), (1, 4)))
    kv_latent = draw_kv_latent(jax.random.fold_in(jax.random.fold_in(seeds[8], part), 71), part)
    doc_ids = jnp.searchsorted(jnp.cumsum(ragged(own_keys[2], DOCS, TOKENS, TOKENS // 2, 0)), jnp.arange(TOKENS), side="right").astype(jnp.int32)
    w_kv = bell_draw(seeds[3], (KVL, HEADS * (NOPE + VDIM)), KVL ** -0.5, 0.25, ((1, 4),))
    w_out = bell_draw(seeds[4], (HEADS * VDIM, D), VDIM ** -0.5, 0.5, ((0, 4),))
    w_enc = bell_draw(seeds[5], (D, KVL + ROPE), D ** -0.5, 0.0625, ((0, 4),))
    residual = draw_residual(jax.random.fold_in(jax.random.fold_in(seeds[8], part), 71), part)
    norm_gain = jnp.clip(1.0 + 0.18 * jax.random.normal(seeds[7], (D,), jnp.float32), 0.1, 1.9)
    return {"queries": queries, "kv_latent": kv_latent, "doc_ids": doc_ids, "w_kv": w_kv, "w_out": w_out, "w_enc": w_enc, "residual": residual, "norm_gain": norm_gain}


masked_score = -1e+30
epsilon = 1e-06

def reference(queries, kv_latent, doc_ids, w_kv, w_out, w_enc, residual, norm_gain):
    count = kv_latent.shape[0]
    content = kv_latent[:, :KVL]
    rotary = kv_latent[:, KVL:]
    positions = jnp.arange(count, dtype=jnp.int32)
    visible = (doc_ids[None, :] == doc_ids[:, None]) & (positions[None, :] <= positions[:, None])
    score_scale = 1.0 / math.sqrt(NOPE + ROPE)
    stacked_w = w_kv.reshape(KVL, HEADS, NOPE + VDIM).transpose(1, 0, 2)
    stacked_q = queries.reshape(count, HEADS, NOPE + ROPE).transpose(1, 0, 2)

    def one_head(paired):
        w_head, q_head = paired
        keys = jnp.dot(content, w_head[:, :NOPE], preferred_element_type=jnp.float32).astype(jnp.bfloat16)
        values = jnp.dot(content, w_head[:, NOPE:], preferred_element_type=jnp.float32).astype(jnp.bfloat16)
        scores = jnp.dot(q_head[:, :NOPE], keys.T, preferred_element_type=jnp.float32)
        scores = scores + jnp.dot(q_head[:, NOPE:], rotary.T, preferred_element_type=jnp.float32)
        scores = jnp.where(visible, scores * score_scale, masked_score)
        highest = lax.optimization_barrier(jnp.max(scores, axis=1, keepdims=True))
        probs = jnp.where(visible, jnp.exp(scores - highest), 0.0)
        total = lax.optimization_barrier(jnp.sum(probs, axis=1, keepdims=True))
        mixed = jnp.dot(probs.astype(jnp.bfloat16), values, preferred_element_type=jnp.float32)
        return (mixed / total).astype(jnp.bfloat16)
    heads_out = lax.map(one_head, (stacked_w, stacked_q))
    attended = heads_out.transpose(1, 0, 2).reshape(count, HEADS * VDIM)
    attn_out = jnp.dot(attended, w_out, preferred_element_type=jnp.float32).astype(jnp.bfloat16)
    hidden = residual.astype(jnp.float32) + attn_out.astype(jnp.float32)
    mean_sq = lax.optimization_barrier(jnp.mean(hidden * hidden, axis=1))
    scaled = (hidden * norm_gain[None, :]).astype(jnp.bfloat16)
    encoded = jnp.dot(scaled, w_enc, preferred_element_type=jnp.float32)
    next_latent = (encoded * lax.rsqrt(mean_sq + epsilon)[:, None]).astype(jnp.bfloat16)
    return (attn_out, next_latent)
```

```python
import functools
import math

import jax
import jax.numpy as jnp
from jax import lax
from jax.experimental import pallas as pl
from jax.experimental.pallas import tpu as pltpu
from jax.sharding import PartitionSpec as P

D = 7168
KVL = 512
ROPE = 64
NOPE = 128
VDIM = 128

LANES = 128
CHUNKS = 7
VMEM_BYTES = 60 * 1024 * 1024
MESH = pl.DeviceIdType.MESH

masked_score = -1e30
epsilon = 1e-06


def kernel(
    n_ctx, n_head, chunks,
    q_hbm, lat_hbm, doc_hbm, wkv_hbm, wout_hbm, wenc_hbm, res_hbm, gain_hbm,
    attn_ref, next_ref,
    q_v, lat_v, doc_v, wkv_v, wout_v, wenc_v, res_v, gain_v,
    lat_all, att_v, s1, r1, s2, r2, enc_s, enc_r, nl_all,
    load_sem, wout_sem, lat_send, lat_recv, s1_send, s1_recv, s2_send, s2_recv,
    enc_send, enc_recv, nl_send, nl_recv,
):
    rows = q_hbm.shape[0]
    heads = wkv_hbm.shape[1] // (NOPE + VDIM)
    width = res_hbm.shape[1]
    part = width // chunks
    piece = rows // n_head
    count = n_ctx * rows
    c = lax.axis_index("ctx")
    h = lax.axis_index("head")
    half = n_head // 2
    near = h + 1 - 2 * lax.rem(h, 2)
    far = lax.rem(h + half, n_head)
    near_far = lax.rem(near + half, n_head)
    slices = (near_far, near, far, h)

    loads = []
    for i, (src, dst) in enumerate((
        (lat_hbm, lat_v), (doc_hbm, doc_v), (q_hbm, q_v), (wkv_hbm, wkv_v),
        (res_hbm, res_v), (wenc_hbm, wenc_v), (gain_hbm, gain_v),
    )):
        loads.append(pltpu.make_async_copy(src, dst, load_sem.at[i]))
    for i in range(4):
        loads[i].start()

    barrier = pltpu.get_barrier_semaphore()
    for step in range(1, n_ctx):
        pl.semaphore_signal(barrier, inc=1, device_id={"ctx": lax.rem(c + step, n_ctx)}, device_id_type=MESH)
    for step in range(1, n_head):
        pl.semaphore_signal(barrier, inc=1, device_id={"head": lax.rem(h + step, n_head)}, device_id_type=MESH)

    wout_loads = []
    for role in range(4):
        for k in range(chunks):
            start = pl.multiple_of(slices[role] * width + k * part, LANES)
            wout_loads.append(pltpu.make_async_copy(
                wout_hbm.at[:, pl.ds(start, part)], wout_v.at[role * chunks + k], wout_sem.at[role * chunks + k]
            ))
            wout_loads[-1].start()
    for i in range(4, 7):
        loads[i].start()

    loads[0].wait()
    loads[1].wait()
    doc_row = jnp.broadcast_to(doc_v[...].astype(jnp.float32), (rows, rows))
    eye = lax.broadcasted_iota(jnp.int32, (rows, rows), 0) == lax.broadcasted_iota(jnp.int32, (rows, rows), 1)
    doc_col = jnp.sum(jnp.where(eye, doc_row, 0.0), axis=1, keepdims=True)
    lat_all[c, :, KVL:] = jnp.broadcast_to(doc_col, (rows, LANES)).astype(jnp.bfloat16)
    lat_all[c, :, : KVL + ROPE] = lat_v[...]
    for src in range(1, n_ctx):
        @pl.when(src > c)
        def _():
            lat_all[src] = jnp.zeros((rows, KVL + LANES), jnp.bfloat16)

    pl.semaphore_wait(barrier, n_ctx - 1 + n_head - 1)

    def latent_copy(step, sender):
        return pltpu.make_async_remote_copy(
            src_ref=lat_all.at[sender], dst_ref=lat_all.at[sender],
            send_sem=lat_send.at[step], recv_sem=lat_recv.at[step],
            device_id={"ctx": lax.rem(c + step, n_ctx)}, device_id_type=MESH,
        )

    for step in range(1, n_ctx):
        @pl.when(c + step < n_ctx)
        def _():
            latent_copy(step, c).start()

    loads[2].wait()
    lane = lax.broadcasted_iota(jnp.int32, (rows, LANES), 1)
    low = lane < ROPE
    q_nope, q_rope = [], []
    for head in range(heads):
        first, shift = divmod(head * (NOPE + ROPE), LANES)
        a = q_v[:, first * LANES : (first + 1) * LANES].astype(jnp.float32)
        b = q_v[:, (first + 1) * LANES : (first + 2) * LANES].astype(jnp.float32)
        if shift:
            a = pltpu.roll(a, shift, 1)
            b = pltpu.roll(b, shift, 1)
            a = jnp.where(low, a, b)
        q_nope.append(a.astype(jnp.bfloat16))
        q_rope.append(jnp.where(low, b, 0.0).astype(jnp.bfloat16))
    loads[3].wait()

    for step in range(1, n_ctx):
        @pl.when(c >= step)
        def _():
            latent_copy(step, lax.rem(c + n_ctx - step, n_ctx)).wait_recv()

    content = lat_all[:, :, :KVL].reshape(count, KVL)
    tail = lat_all[:, :, KVL:].reshape(count, LANES)
    nt = (((1,), (1,)), ((), ()))
    pick = (lax.broadcasted_iota(jnp.int32, (16, LANES), 1) == ROPE).astype(jnp.float32).astype(jnp.bfloat16)
    key_docs = lax.dot_general(pick, tail, nt, preferred_element_type=jnp.float32)[0:1]
    key_pos = lax.broadcasted_iota(jnp.int32, (rows, count), 1)
    row_pos = lax.broadcasted_iota(jnp.int32, (rows, count), 0) + c * rows
    visible = (jnp.broadcast_to(key_docs, (rows, count)) == jnp.broadcast_to(doc_col, (rows, count))) & (key_pos <= row_pos)
    score_scale = 1.0 / math.sqrt(NOPE + ROPE)
    both = NOPE + VDIM
    for head in range(heads):
        kv = jnp.dot(
            content, wkv_v[:, head * both : (head + 1) * both], preferred_element_type=jnp.float32
        ).astype(jnp.bfloat16)
        scores = lax.dot_general(q_nope[head], kv[:, :NOPE], nt, preferred_element_type=jnp.float32)
        scores = scores + lax.dot_general(q_rope[head], tail, nt, preferred_element_type=jnp.float32)
        scores = jnp.where(visible, scores * score_scale, masked_score)
        highest = jnp.max(scores, axis=1, keepdims=True)
        probs = jnp.where(visible, jnp.exp(scores - highest), 0.0)
        total = jnp.sum(probs, axis=1, keepdims=True)
        mixed = jnp.dot(probs.astype(jnp.bfloat16), kv[:, NOPE:], preferred_element_type=jnp.float32)
        att_v[:, head * VDIM : (head + 1) * VDIM] = (mixed / total).astype(jnp.bfloat16)

    att = att_v[...]

    def partial_of(role, k):
        slot = role * chunks + k
        wout_loads[slot].wait()
        return jnp.dot(att, wout_v[slot], preferred_element_type=jnp.float32)

    first = []
    for role in range(2):
        for k in range(chunks):
            slot = role * chunks + k
            s1[slot] = partial_of(role, k).astype(jnp.bfloat16)
            copy = pltpu.make_async_remote_copy(
                src_ref=s1.at[slot], dst_ref=r1.at[slot],
                send_sem=s1_send.at[slot], recv_sem=s1_recv.at[slot],
                device_id={"head": near}, device_id_type=MESH,
            )
            copy.start()
            first.append(copy)

    second = []
    for k in range(chunks):
        mine = partial_of(2, k)
        first[k].wait_recv()
        s2[k] = (mine + r1[k].astype(jnp.float32)).astype(jnp.bfloat16)
        copy = pltpu.make_async_remote_copy(
            src_ref=s2.at[k], dst_ref=r2.at[k],
            send_sem=s2_send.at[k], recv_sem=s2_recv.at[k],
            device_id={"head": far}, device_id_type=MESH,
        )
        copy.start()
        second.append(copy)

    for i in range(4, 7):
        loads[i].wait()
    encoded = jnp.zeros((rows, KVL + ROPE), jnp.float32)
    squares = jnp.zeros((rows, 1), jnp.float32)
    for k in range(chunks):
        cols = slice(k * part, (k + 1) * part)
        mine = partial_of(3, k)
        first[chunks + k].wait_recv()
        mine = mine + r1[chunks + k].astype(jnp.float32)
        second[k].wait_recv()
        out = (mine + r2[k].astype(jnp.float32)).astype(jnp.bfloat16)
        attn_ref[:, cols] = out
        hidden = res_v[:, cols].astype(jnp.float32) + out.astype(jnp.float32)
        squares = squares + jnp.sum(hidden * hidden, axis=1, keepdims=True)
        scaled = (hidden * gain_v[cols][None]).astype(jnp.bfloat16)
        encoded = encoded + lax.dot_general(
            scaled, wenc_v[:, cols], nt, preferred_element_type=jnp.float32
        )

    coarse = squares.astype(jnp.bfloat16).astype(jnp.float32)
    fine = squares - coarse
    split = ROPE + (LANES - ROPE) // 2
    sums = jnp.where(lane < split, jnp.broadcast_to(coarse, (rows, LANES)), jnp.broadcast_to(fine, (rows, LANES)))
    enc_s[:, :, KVL:] = sums.astype(jnp.bfloat16).reshape(n_head, piece, LANES)
    enc_s[:, :, : KVL + ROPE] = encoded.astype(jnp.bfloat16).reshape(n_head, piece, KVL + ROPE)
    enc_copies = []
    for step in range(1, n_head):
        peer = lax.rem(h + step, n_head)
        copy = pltpu.make_async_remote_copy(
            src_ref=enc_s.at[peer], dst_ref=enc_r.at[step - 1],
            send_sem=enc_send.at[step - 1], recv_sem=enc_recv.at[step - 1],
            device_id={"head": peer}, device_id_type=MESH,
        )
        copy.start()
        enc_copies.append(copy)
    whole = enc_s[h].astype(jnp.float32)
    for step in range(1, n_head):
        enc_copies[step - 1].wait_recv()
        whole = whole + enc_r[step - 1].astype(jnp.float32)
    square_sum = whole[:, KVL + ROPE : KVL + ROPE + 1] + whole[:, KVL + split : KVL + split + 1]
    scale = lax.rsqrt(square_sum / (width * n_head) + epsilon)
    nl_all[h] = (whole[:, : KVL + ROPE] * scale).astype(jnp.bfloat16)
    nl_copies = []
    for step in range(1, n_head):
        copy = pltpu.make_async_remote_copy(
            src_ref=nl_all.at[h], dst_ref=nl_all.at[h],
            send_sem=nl_send.at[step - 1], recv_sem=nl_recv.at[step - 1],
            device_id={"head": lax.rem(h + step, n_head)}, device_id_type=MESH,
        )
        copy.start()
        nl_copies.append(copy)
    for copy in nl_copies:
        copy.wait_recv()
    next_ref[...] = nl_all[...].reshape(rows, KVL + ROPE)

    for step in range(1, n_ctx):
        @pl.when(c + step < n_ctx)
        def _():
            latent_copy(step, c).wait_send()
    for copy in first + second + enc_copies + nl_copies:
        copy.wait_send()


def fused(n_ctx, n_head, queries, kv_latent, doc_ids, w_kv, w_out, w_enc, residual, norm_gain):
    rows = queries.shape[0]
    heads = w_kv.shape[1] // (NOPE + VDIM)
    width = residual.shape[1]
    part = width // CHUNKS
    piece = rows // n_head
    bf16, f32 = jnp.bfloat16, jnp.float32
    hbm = pl.BlockSpec(memory_space=pltpu.HBM)
    vmem = pl.BlockSpec(memory_space=pltpu.VMEM)
    dma = pltpu.SemaphoreType.DMA
    return pl.pallas_call(
        functools.partial(kernel, n_ctx, n_head, CHUNKS),
        out_shape=(pltpu.VMEM((rows, width), bf16), pltpu.VMEM((rows, KVL + ROPE), bf16)),
        in_specs=[hbm] * 8,
        out_specs=(vmem, vmem),
        scratch_shapes=[
            pltpu.VMEM(queries.shape, bf16),
            pltpu.VMEM(kv_latent.shape, bf16),
            pltpu.VMEM((1, rows), jnp.int32),
            pltpu.VMEM(w_kv.shape, bf16),
            pltpu.VMEM((4 * CHUNKS, w_out.shape[0], part), bf16),
            pltpu.VMEM(w_enc.shape[::-1], bf16),
            pltpu.VMEM(residual.shape, bf16),
            pltpu.VMEM((width,), f32),
            pltpu.VMEM((n_ctx, rows, KVL + LANES), bf16),
            pltpu.VMEM((rows, heads * VDIM), bf16),
            pltpu.VMEM((2 * CHUNKS, rows, part), bf16),
            pltpu.VMEM((2 * CHUNKS, rows, part), bf16),
            pltpu.VMEM((CHUNKS, rows, part), bf16),
            pltpu.VMEM((CHUNKS, rows, part), bf16),
            pltpu.VMEM((n_head, piece, KVL + LANES), bf16),
            pltpu.VMEM((n_head - 1, piece, KVL + LANES), bf16),
            pltpu.VMEM((n_head, piece, KVL + ROPE), bf16),
            dma((7,)),
            dma((4 * CHUNKS,)),
            dma((n_ctx,)),
            dma((n_ctx,)),
            dma((2 * CHUNKS,)),
            dma((2 * CHUNKS,)),
            dma((CHUNKS,)),
            dma((CHUNKS,)),
            dma((n_head - 1,)),
            dma((n_head - 1,)),
            dma((n_head - 1,)),
            dma((n_head - 1,)),
        ],
        compiler_params=pltpu.CompilerParams(
            collective_id=0, has_side_effects=True, vmem_limit_bytes=VMEM_BYTES
        ),
        name="latent_layer",
    )(
        queries, kv_latent, doc_ids[None], w_kv, w_out, w_enc.T, residual, norm_gain,
    )


def general(n_ctx, n_head, queries, kv_latent, doc_ids, w_kv, w_out, w_enc, residual, norm_gain):
    rows_here = queries.shape[0]
    heads_here = w_kv.shape[1] // (NOPE + VDIM)
    query_heads = queries.reshape(rows_here, heads_here, NOPE + ROPE)
    q_nope = query_heads[:, :, :NOPE]
    q_rope = query_heads[:, :, NOPE:]
    positions = lax.axis_index("ctx") * rows_here + lax.iota(jnp.int32, rows_here)
    weights = w_kv.reshape(KVL, heads_here, NOPE + VDIM)
    f32 = jnp.float32
    latents = lax.all_gather(kv_latent, "ctx", axis=0, tiled=True)
    key_docs = lax.all_gather(doc_ids, "ctx", axis=0, tiled=True)
    key_pos = lax.iota(jnp.int32, latents.shape[0])
    content = latents[:, :KVL]
    rotary = latents[:, KVL:]
    both = jnp.einsum("nc,chd->nhd", content, weights, preferred_element_type=f32).astype(jnp.bfloat16)
    keys = both[:, :, :NOPE]
    values = both[:, :, NOPE:]
    scores = jnp.einsum("qhd,nhd->hqn", q_nope, keys, preferred_element_type=f32)
    scores = scores + jnp.einsum("qhd,nd->hqn", q_rope, rotary, preferred_element_type=f32)
    visible = (key_docs[None, :] == doc_ids[:, None]) & (key_pos[None, :] <= positions[:, None])
    scores = jnp.where(visible[None], scores * (1.0 / math.sqrt(NOPE + ROPE)), masked_score)
    highest = jnp.max(scores, axis=2)
    probs = jnp.where(visible[None], jnp.exp(scores - highest[:, :, None]), 0.0)
    total = jnp.sum(probs, axis=2)
    mixed = jnp.einsum("hqn,nhd->hqd", probs.astype(jnp.bfloat16), values, preferred_element_type=f32)
    attended = (mixed / total[:, :, None]).astype(jnp.bfloat16)
    side_by_side = attended.transpose(1, 0, 2).reshape(rows_here, heads_here * VDIM)
    summed = lax.psum_scatter(
        lax.dot_general(w_out, side_by_side, (((0,), (1,)), ((), ())), preferred_element_type=f32),
        "head", scatter_dimension=0, tiled=True,
    )
    attn_out = summed.T.astype(jnp.bfloat16)
    hidden = residual.astype(f32) + attn_out.astype(f32)
    squares = jnp.sum(hidden * hidden, axis=1)
    scaled = (hidden * norm_gain[None, :]).astype(jnp.bfloat16)
    encoded = jnp.dot(scaled, w_enc, preferred_element_type=f32)
    enc_sum, sq_sum = lax.psum((encoded, squares), "head")
    next_latent = (enc_sum * lax.rsqrt(sq_sum / D + epsilon)[:, None]).astype(jnp.bfloat16)
    return (attn_out, next_latent)


def per_device(n_ctx, n_head, *args):
    rows, width = args[6].shape
    whole_tiles = width % (CHUNKS * LANES) == 0 and rows % (16 * n_head) == 0
    body = fused if n_head == 4 and whole_tiles else general
    return body(n_ctx, n_head, *args)


def solution(mesh):
    return jax.shard_map(
        functools.partial(per_device, mesh.shape["ctx"], mesh.shape["head"]),
        mesh=mesh,
        in_specs=(
            P(("rep", "ctx"), "head"),
            P(("rep", "ctx"), None),
            P(("rep", "ctx")),
            P(None, "head"),
            P("head", None),
            P("head", None),
            P(("rep", "ctx"), "head"),
            P("head"),
        ),
        out_specs=(P(("rep", "ctx"), "head"), P(("rep", "ctx"), None)),
        check_vma=False,
    )
```

```python
import functools
import math

import jax
import jax.numpy as jnp
from jax import lax
from jax.experimental import pallas as pl
from jax.experimental.pallas import tpu as pltpu
from jax.sharding import PartitionSpec as P

D = 7168
KVL = 512
ROPE = 64
NOPE = 128
VDIM = 128

LANES = 128
CHUNKS = 7
PIECE = 16
VMEM_BYTES = 60 * 1024 * 1024
MESH = pl.DeviceIdType.MESH

masked_score = -1e30
epsilon = 1e-06


def kernel(
    n_ctx, n_head, back, chunks,
    q_hbm, lat_hbm, doc_hbm, wkv_hbm, wout_hbm, wenc_hbm, res_hbm, gain_hbm,
    attn_ref, next_ref,
    q_v, lat_v, doc_v, wkv_v, wout_v, wenc_v, res_v, gain_v,
    lat_all, att_v, sums_s, sums_r, enc_s, enc_r,
    load_sem, wout_sem, lat_send, lat_recv, sums_send, sums_recv,
    enc_send, enc_recv,
):
    rows = q_hbm.shape[0]
    heads = wkv_hbm.shape[1] // (NOPE + VDIM)
    width = res_hbm.shape[1]
    part = width // chunks
    pieces = rows // PIECE
    c = lax.axis_index("ctx")
    h = lax.axis_index("head")
    side = h // 2
    end, mate = 3 * side, 1 + side
    partner = h + 1 - 2 * lax.rem(h, 2)
    other = 3 - mate
    at_end = h == end
    at_mate = h == mate
    far_end = 3 - end
    slices = (far_end, other, partner, h)

    loads = []
    for i, (src, dst) in enumerate((
        (lat_hbm, lat_v), (doc_hbm, doc_v), (q_hbm, q_v), (wkv_hbm, wkv_v),
        (res_hbm, res_v), (wenc_hbm, wenc_v), (gain_hbm, gain_v),
    )):
        loads.append(pltpu.make_async_copy(src, dst, load_sem.at[i]))
    for i in range(4):
        loads[i].start()

    barrier = pltpu.get_barrier_semaphore()
    near = [("ctx", c, step, n_ctx) for step in range(1, back + 1)] + [("head", h, 1, n_head)]
    for axis, here, step, count in near:
        @pl.when(here + step < count)
        def _():
            pl.semaphore_signal(barrier, inc=1, device_id={axis: here + step}, device_id_type=MESH)

        @pl.when(here >= step)
        def _():
            pl.semaphore_signal(barrier, inc=1, device_id={axis: here - step}, device_id_type=MESH)

    for role in range(4):
        for k in range(chunks):
            start = pl.multiple_of(slices[role] * width + k * part, LANES)
            pltpu.make_async_copy(
                wout_hbm.at[:, pl.ds(start, part)], wout_v.at[role, k], wout_sem.at[role]
            ).start()
    for i in range(4, 7):
        loads[i].start()

    loads[0].wait()
    loads[1].wait()
    docs_here = doc_v[...].astype(jnp.float32)
    row_of = lax.broadcasted_iota(jnp.int32, (rows, rows), 0)
    col_of = lax.broadcasted_iota(jnp.int32, (rows, rows), 1)
    doc_col = jnp.sum(
        jnp.where(row_of == col_of, jnp.broadcast_to(docs_here, (rows, rows)), 0.0), axis=1, keepdims=True
    )
    lat_all[back, :, KVL:] = jnp.broadcast_to(doc_col, (rows, LANES)).astype(jnp.bfloat16)
    lat_all[back, :, : KVL + ROPE] = lat_v[...]
    for step in range(1, back + 1):
        @pl.when(c < step)
        def _():
            lat_all[back - step] = jnp.zeros((rows, KVL + LANES), jnp.bfloat16)

    peers = 0
    for axis, here, step, count in near:
        peers = peers + (here + step < count).astype(jnp.int32) + (here >= step).astype(jnp.int32)
    pl.semaphore_wait(barrier, peers)

    def latent_copy(step):
        return pltpu.make_async_remote_copy(
            src_ref=lat_all.at[back], dst_ref=lat_all.at[back - step],
            send_sem=lat_send.at[step - 1], recv_sem=lat_recv.at[step - 1],
            device_id={"ctx": lax.rem(c + step, n_ctx)}, device_id_type=MESH,
        )

    for step in range(1, back + 1):
        @pl.when(c + step < n_ctx)
        def _():
            latent_copy(step).start()

    loads[2].wait()
    low = lax.broadcasted_iota(jnp.int32, (rows, LANES), 1) < ROPE
    query = []
    for head in range(heads):
        first, shift = divmod(head * (NOPE + ROPE), LANES)
        a = q_v[:, first * LANES : (first + 1) * LANES].astype(jnp.float32)
        b = q_v[:, (first + 1) * LANES : (first + 2) * LANES].astype(jnp.float32)
        if shift:
            a = pltpu.roll(a, shift, 1)
            b = pltpu.roll(b, shift, 1)
            a = jnp.where(low, a, b)
        query.append(jnp.concatenate([a, jnp.where(low, b, 0.0)], axis=1).astype(jnp.bfloat16))
    loads[3].wait()

    nt = (((1,), (1,)), ((), ()))
    score_scale = 1.0 / math.sqrt(NOPE + ROPE)
    both = NOPE + VDIM

    def expand(latent):
        return jnp.dot(latent, wkv_v[...], preferred_element_type=jnp.float32).astype(jnp.bfloat16)

    def score(expanded, tail, visible):
        found = []
        for head in range(heads):
            keys = jnp.concatenate([expanded[:, head * both : head * both + NOPE], tail], axis=1)
            one = lax.dot_general(query[head], keys, nt, preferred_element_type=jnp.float32)
            found.append(jnp.where(visible, one * score_scale, masked_score))
        return found

    seen_own = (jnp.broadcast_to(docs_here, (rows, rows)) == jnp.broadcast_to(doc_col, (rows, rows))) & (col_of <= row_of)
    kv_own = expand(lat_v[:, :KVL])
    own = score(kv_own, lat_all[back, :, KVL:], seen_own)

    for step in range(1, back + 1):
        @pl.when(c >= step)
        def _():
            latent_copy(step).wait_recv()

    count = back * rows
    tail_prev = lat_all[:back, :, KVL:].reshape(count, LANES)
    pick = (lax.broadcasted_iota(jnp.int32, (16, LANES), 1) == ROPE).astype(jnp.float32).astype(jnp.bfloat16)
    key_docs = lax.dot_general(pick, tail_prev, nt, preferred_element_type=jnp.float32)[0:1]
    exists = lax.broadcasted_iota(jnp.int32, (rows, count), 1) + (c - back) * rows >= 0
    seen_prev = (jnp.broadcast_to(key_docs, (rows, count)) == jnp.broadcast_to(doc_col, (rows, count))) & exists
    kv_prev = expand(lat_all[:back, :, :KVL].reshape(count, KVL))
    prev = score(kv_prev, tail_prev, seen_prev)
    for head in range(heads):
        highest = jnp.maximum(
            jnp.max(own[head], axis=1, keepdims=True), jnp.max(prev[head], axis=1, keepdims=True)
        )
        p_own = jnp.where(seen_own, jnp.exp(own[head] - highest), 0.0)
        p_prev = jnp.where(seen_prev, jnp.exp(prev[head] - highest), 0.0)
        total = jnp.sum(p_own, axis=1, keepdims=True) + jnp.sum(p_prev, axis=1, keepdims=True)
        columns = slice(head * both + NOPE, (head + 1) * both)
        mixed = jnp.dot(p_own.astype(jnp.bfloat16), kv_own[:, columns], preferred_element_type=jnp.float32)
        mixed = mixed + jnp.dot(p_prev.astype(jnp.bfloat16), kv_prev[:, columns], preferred_element_type=jnp.float32)
        att_v[:, head * VDIM : (head + 1) * VDIM] = (mixed / total).astype(jnp.bfloat16)

    def partial_of(role, k):
        if k == 0:
            pltpu.make_async_copy(wout_v.at[role], wout_v.at[role], wout_sem.at[role]).wait()
        return jnp.dot(att_v[...], wout_v[role, k], preferred_element_type=jnp.float32)

    def sums_copy(slot, landing, device):
        return pltpu.make_async_remote_copy(
            src_ref=sums_s.at[slot], dst_ref=sums_r.at[landing],
            send_sem=sums_send, recv_sem=sums_recv.at[landing],
            device_id={"head": device}, device_id_type=MESH,
        )

    def piece_copy(piece, landing, device):
        return pltpu.make_async_remote_copy(
            src_ref=enc_s.at[piece], dst_ref=enc_r.at[landing],
            send_sem=enc_send, recv_sem=enc_recv.at[landing],
            device_id={"head": device}, device_id_type=MESH,
        )

    def finish(k, out, encoded, squares):
        cols = slice(k * part, (k + 1) * part)
        attn_ref[:, cols] = out
        hidden = res_v[:, cols].astype(jnp.float32) + out.astype(jnp.float32)
        squares = squares + jnp.sum(hidden * hidden, axis=1, keepdims=True)
        scaled = (hidden * gain_v[cols][None]).astype(jnp.bfloat16)
        encoded = encoded + lax.dot_general(scaled, wenc_v[:, cols], nt, preferred_element_type=jnp.float32)
        return encoded, squares

    split = ROPE + (LANES - ROPE) // 2
    coarse_lanes = lax.broadcasted_iota(jnp.int32, (PIECE, LANES), 1) < split

    def pack(piece, encoded, squares):
        coarse = squares.astype(jnp.bfloat16).astype(jnp.float32)
        sums = jnp.where(
            coarse_lanes,
            jnp.broadcast_to(coarse, (PIECE, LANES)), jnp.broadcast_to(squares - coarse, (PIECE, LANES)),
        )
        enc_s[piece, :, KVL:] = sums.astype(jnp.bfloat16)
        enc_s[piece, :, : KVL + ROPE] = encoded.astype(jnp.bfloat16)

    def unpack(packed):
        squares = packed[:, KVL + ROPE : KVL + ROPE + 1] + packed[:, KVL + split : KVL + split + 1]
        return packed[:, : KVL + ROPE], squares

    def conclude(near_half):
        for piece in range(pieces):
            if near_half is None:
                piece_copy(piece, piece, partner).wait_recv()
            piece_copy(piece, pieces + piece, other).wait_recv()
            near = (enc_r[piece] if near_half is None else near_half[piece]).astype(jnp.float32)
            whole, square_sum = unpack(near + enc_r[pieces + piece].astype(jnp.float32))
            scale = lax.rsqrt(square_sum / (width * n_head) + epsilon)
            next_ref[piece * PIECE : (piece + 1) * PIECE, :] = (whole * scale).astype(jnp.bfloat16)

    for i in range(4, 7):
        loads[i].wait()
    nothing = jnp.zeros((rows, KVL + ROPE), jnp.float32), jnp.zeros((rows, 1), jnp.float32)

    @pl.when(at_end)
    def _():
        for slot in range(3 * chunks):
            role, k = divmod(slot, chunks)
            sums_s[slot] = partial_of(role, k).astype(jnp.bfloat16)
            sums_copy(slot, slot, partner).start()
        encoded, squares = nothing
        for k in range(chunks):
            mine = partial_of(3, k)
            sums_copy(k, k, partner).wait_recv()
            out = (mine + sums_r[k].astype(jnp.float32)).astype(jnp.bfloat16)
            encoded, squares = finish(k, out, encoded, squares)
        for piece in range(pieces):
            own_rows = slice(piece * PIECE, (piece + 1) * PIECE)
            pack(piece, encoded[own_rows], squares[own_rows])
            piece_copy(piece, piece, partner).start()
        conclude(None)

    @pl.when(at_mate)
    def _():
        lag = 3
        for slot in range(2 * chunks):
            role, k = divmod(slot, chunks)
            mine = partial_of(role, k)
            sums_copy(slot, slot, partner).wait_recv()
            sums_s[slot] = (mine + sums_r[slot].astype(jnp.float32)).astype(jnp.bfloat16)
            sums_copy(slot, 3 * chunks + slot, other).start()
            k = slot - lag
            if 0 <= k < chunks:
                mine = partial_of(2, k)
                landed = 3 * chunks + k
                sums_copy(k, landed, other).wait_recv()
                sums_s[2 * chunks + k] = (mine + sums_r[landed].astype(jnp.float32)).astype(jnp.bfloat16)
                sums_copy(2 * chunks + k, k, partner).start()
        encoded, squares = nothing
        for k in range(chunks):
            mine = partial_of(3, k)
            landed = 4 * chunks + k
            sums_copy(k, landed, other).wait_recv()
            mine = mine + sums_r[landed].astype(jnp.float32)
            sums_copy(k, 2 * chunks + k, partner).wait_recv()
            out = (mine + sums_r[2 * chunks + k].astype(jnp.float32)).astype(jnp.bfloat16)
            encoded, squares = finish(k, out, encoded, squares)
        for piece in range(pieces):
            own_rows = slice(piece * PIECE, (piece + 1) * PIECE)
            piece_copy(piece, piece, partner).wait_recv()
            theirs, their_squares = unpack(enc_r[piece].astype(jnp.float32))
            pack(piece, encoded[own_rows] + theirs, squares[own_rows] + their_squares)
            piece_copy(piece, pieces + piece, far_end).start()
            piece_copy(piece, piece, partner).start()
        for piece in range(pieces):
            piece_copy(piece, pieces + piece, other).start()
        conclude(enc_s)

    for step in range(1, back + 1):
        @pl.when(c + step < n_ctx)
        def _():
            latent_copy(step).wait_send()
    all_sums = pltpu.make_async_copy(sums_s, sums_s, sums_send)
    all_sums.wait()
    all_pieces = pltpu.make_async_copy(enc_s, enc_s, enc_send)

    @pl.when(at_end)
    def _():
        all_pieces.wait()

    @pl.when(at_mate)
    def _():
        for _ in range(3):
            all_pieces.wait()


def fused(n_ctx, n_head, queries, kv_latent, doc_ids, w_kv, w_out, w_enc, residual, norm_gain):
    rows = queries.shape[0]
    heads = w_kv.shape[1] // (NOPE + VDIM)
    width = residual.shape[1]
    part = width // CHUNKS
    pieces = rows // PIECE
    back = min(n_ctx - 1, -(-(n_ctx * rows // 2 - 1) // rows))
    bf16, f32 = jnp.bfloat16, jnp.float32
    hbm = pl.BlockSpec(memory_space=pltpu.HBM)
    vmem = pl.BlockSpec(memory_space=pltpu.VMEM)
    dma = pltpu.SemaphoreType.DMA
    return pl.pallas_call(
        functools.partial(kernel, n_ctx, n_head, back, CHUNKS),
        out_shape=(pltpu.VMEM((rows, width), bf16), pltpu.VMEM((rows, KVL + ROPE), bf16)),
        in_specs=[hbm] * 8,
        out_specs=(vmem, vmem),
        scratch_shapes=[
            pltpu.VMEM(queries.shape, bf16),
            pltpu.VMEM(kv_latent.shape, bf16),
            pltpu.VMEM((1, rows), jnp.int32),
            pltpu.VMEM(w_kv.shape, bf16),
            pltpu.VMEM((4, CHUNKS, w_out.shape[0], part), bf16),
            pltpu.VMEM(w_enc.shape[::-1], bf16),
            pltpu.VMEM(residual.shape, bf16),
            pltpu.VMEM((width,), f32),
            pltpu.VMEM((back + 1, rows, KVL + LANES), bf16),
            pltpu.VMEM((rows, heads * VDIM), bf16),
            pltpu.VMEM((3 * CHUNKS, rows, part), bf16),
            pltpu.VMEM((5 * CHUNKS, rows, part), bf16),
            pltpu.VMEM((pieces, PIECE, KVL + LANES), bf16),
            pltpu.VMEM((2 * pieces, PIECE, KVL + LANES), bf16),
            dma((7,)),
            dma((4,)),
            dma((back,)),
            dma((back,)),
            dma,
            dma((5 * CHUNKS,)),
            dma,
            dma((2 * pieces,)),
        ],
        compiler_params=pltpu.CompilerParams(
            collective_id=0, has_side_effects=True, vmem_limit_bytes=VMEM_BYTES
        ),
        name="latent_layer",
    )(
        queries, kv_latent, doc_ids[None], w_kv, w_out, w_enc.T, residual, norm_gain,
    )


def general(n_ctx, n_head, queries, kv_latent, doc_ids, w_kv, w_out, w_enc, residual, norm_gain):
    rows_here = queries.shape[0]
    heads_here = w_kv.shape[1] // (NOPE + VDIM)
    query_heads = queries.reshape(rows_here, heads_here, NOPE + ROPE)
    q_nope = query_heads[:, :, :NOPE]
    q_rope = query_heads[:, :, NOPE:]
    positions = lax.axis_index("ctx") * rows_here + lax.iota(jnp.int32, rows_here)
    weights = w_kv.reshape(KVL, heads_here, NOPE + VDIM)
    f32 = jnp.float32
    latents = lax.all_gather(kv_latent, "ctx", axis=0, tiled=True)
    key_docs = lax.all_gather(doc_ids, "ctx", axis=0, tiled=True)
    key_pos = lax.iota(jnp.int32, latents.shape[0])
    content = latents[:, :KVL]
    rotary = latents[:, KVL:]
    both = jnp.einsum("nc,chd->nhd", content, weights, preferred_element_type=f32).astype(jnp.bfloat16)
    keys = both[:, :, :NOPE]
    values = both[:, :, NOPE:]
    scores = jnp.einsum("qhd,nhd->hqn", q_nope, keys, preferred_element_type=f32)
    scores = scores + jnp.einsum("qhd,nd->hqn", q_rope, rotary, preferred_element_type=f32)
    visible = (key_docs[None, :] == doc_ids[:, None]) & (key_pos[None, :] <= positions[:, None])
    scores = jnp.where(visible[None], scores * (1.0 / math.sqrt(NOPE + ROPE)), masked_score)
    highest = jnp.max(scores, axis=2)
    probs = jnp.where(visible[None], jnp.exp(scores - highest[:, :, None]), 0.0)
    total = jnp.sum(probs, axis=2)
    mixed = jnp.einsum("hqn,nhd->hqd", probs.astype(jnp.bfloat16), values, preferred_element_type=f32)
    attended = (mixed / total[:, :, None]).astype(jnp.bfloat16)
    side_by_side = attended.transpose(1, 0, 2).reshape(rows_here, heads_here * VDIM)
    summed = lax.psum_scatter(
        lax.dot_general(w_out, side_by_side, (((0,), (1,)), ((), ())), preferred_element_type=f32),
        "head", scatter_dimension=0, tiled=True,
    )
    attn_out = summed.T.astype(jnp.bfloat16)
    hidden = residual.astype(f32) + attn_out.astype(f32)
    squares = jnp.sum(hidden * hidden, axis=1)
    scaled = (hidden * norm_gain[None, :]).astype(jnp.bfloat16)
    encoded = jnp.dot(scaled, w_enc, preferred_element_type=f32)
    enc_sum, sq_sum = lax.psum((encoded, squares), "head")
    next_latent = (enc_sum * lax.rsqrt(sq_sum / D + epsilon)[:, None]).astype(jnp.bfloat16)
    return (attn_out, next_latent)


def per_device(n_ctx, n_head, *args):
    rows, width = args[6].shape
    whole_tiles = width % (CHUNKS * LANES) == 0 and rows % PIECE == 0 and rows <= LANES
    body = fused if n_head == 4 and whole_tiles else general
    return body(n_ctx, n_head, *args)


def solution(mesh):
    return jax.shard_map(
        functools.partial(per_device, mesh.shape["ctx"], mesh.shape["head"]),
        mesh=mesh,
        in_specs=(
            P(("rep", "ctx"), "head"),
            P(("rep", "ctx"), None),
            P(("rep", "ctx")),
            P(None, "head"),
            P("head", None),
            P("head", None),
            P(("rep", "ctx"), "head"),
            P("head"),
        ),
        out_specs=(P(("rep", "ctx"), "head"), P(("rep", "ctx"), None)),
        check_vma=False,
    )
```

```python
import functools
import math

import jax
import jax.numpy as jnp
from jax import lax
from jax.experimental import pallas as pl
from jax.experimental.pallas import tpu as pltpu
from jax.sharding import PartitionSpec as P

D = 7168
KVL = 512
ROPE = 64
NOPE = 128
VDIM = 128

LANES = 128
CHUNKS = 7
PIECE = 16
VMEM_BYTES = 60 * 1024 * 1024
MESH = pl.DeviceIdType.MESH

masked_score = -1e30
epsilon = 1e-06


def kernel(
    n_ctx, n_head, back, chunks,
    q_hbm, lat_hbm, doc_hbm, wkv_hbm, wout_hbm, wenc_hbm, res_hbm, gain_hbm,
    attn_ref, next_ref,
    q_v, lat_v, doc_v, wkv_v, wout_v, wenc_v, res_v, gain_v,
    lat_all, att_v, sums_s, sums_r, enc_s, enc_r,
    load_sem, wout_sem, lat_send, lat_recv, sums_send, sums_recv,
    enc_send, enc_recv, far_in,
):
    rows = q_hbm.shape[0]
    heads = wkv_hbm.shape[1] // (NOPE + VDIM)
    width = res_hbm.shape[1]
    part = width // chunks
    pieces = rows // PIECE
    c = lax.axis_index("ctx")
    h = lax.axis_index("head")
    side = h // 2
    end, mate = 3 * side, 1 + side
    partner = h + 1 - 2 * lax.rem(h, 2)
    other = 3 - mate
    at_end = h == end
    at_mate = h == mate
    far_end = 3 - end
    slices = (far_end, other, partner, h)

    loads = []
    for i, (src, dst) in enumerate((
        (lat_hbm, lat_v), (doc_hbm, doc_v), (q_hbm, q_v), (wkv_hbm, wkv_v),
        (res_hbm, res_v), (wenc_hbm, wenc_v), (gain_hbm, gain_v),
    )):
        loads.append(pltpu.make_async_copy(src, dst, load_sem.at[i]))
    for i in range(4):
        loads[i].start()

    barrier = pltpu.get_barrier_semaphore()
    near = [("ctx", c, step, n_ctx) for step in range(1, back + 1)] + [("head", h, 1, n_head)]
    for axis, here, step, count in near:
        @pl.when(here + step < count)
        def _():
            pl.semaphore_signal(barrier, inc=1, device_id={axis: here + step}, device_id_type=MESH)

        @pl.when(here >= step)
        def _():
            pl.semaphore_signal(barrier, inc=1, device_id={axis: here - step}, device_id_type=MESH)

    for role in range(4):
        for k in range(chunks):
            start = pl.multiple_of(slices[role] * width + k * part, LANES)
            pltpu.make_async_copy(
                wout_hbm.at[:, pl.ds(start, part)], wout_v.at[role, k], wout_sem.at[role]
            ).start()
    for i in range(4, 7):
        loads[i].start()

    loads[0].wait()
    loads[1].wait()
    docs_here = doc_v[...].astype(jnp.float32)
    row_of = lax.broadcasted_iota(jnp.int32, (rows, rows), 0)
    col_of = lax.broadcasted_iota(jnp.int32, (rows, rows), 1)
    doc_col = jnp.sum(
        jnp.where(row_of == col_of, jnp.broadcast_to(docs_here, (rows, rows)), 0.0), axis=1, keepdims=True
    )
    lat_all[back, :, KVL:] = jnp.broadcast_to(doc_col, (rows, LANES)).astype(jnp.bfloat16)
    lat_all[back, :, : KVL + ROPE] = lat_v[...]
    for step in range(1, back + 1):
        @pl.when(c < step)
        def _():
            lat_all[back - step] = jnp.zeros((rows, KVL + LANES), jnp.bfloat16)

    peers = 0
    for axis, here, step, count in near:
        peers = peers + (here + step < count).astype(jnp.int32) + (here >= step).astype(jnp.int32)
    pl.semaphore_wait(barrier, peers)

    @pl.when(at_mate)
    def _():
        pl.semaphore_signal(far_in, inc=1, device_id={"head": other}, device_id_type=MESH)


    def latent_copy(step):
        return pltpu.make_async_remote_copy(
            src_ref=lat_all.at[back], dst_ref=lat_all.at[back - step],
            send_sem=lat_send.at[step - 1], recv_sem=lat_recv.at[step - 1],
            device_id={"ctx": lax.rem(c + step, n_ctx)}, device_id_type=MESH,
        )

    for step in range(1, back + 1):
        @pl.when(c + step < n_ctx)
        def _():
            latent_copy(step).start()

    loads[2].wait()
    low = lax.broadcasted_iota(jnp.int32, (rows, LANES), 1) < ROPE
    query = []
    for head in range(heads):
        first, shift = divmod(head * (NOPE + ROPE), LANES)
        a = q_v[:, first * LANES : (first + 1) * LANES].astype(jnp.float32)
        b = q_v[:, (first + 1) * LANES : (first + 2) * LANES].astype(jnp.float32)
        if shift:
            a = pltpu.roll(a, shift, 1)
            b = pltpu.roll(b, shift, 1)
            a = jnp.where(low, a, b)
        query.append(jnp.concatenate([a, jnp.where(low, b, 0.0)], axis=1).astype(jnp.bfloat16))
    loads[3].wait()

    nt = (((1,), (1,)), ((), ()))
    score_scale = 1.0 / math.sqrt(NOPE + ROPE)
    both = NOPE + VDIM

    def expand(latent):
        return jnp.dot(latent, wkv_v[...], preferred_element_type=jnp.float32).astype(jnp.bfloat16)

    def score(expanded, tail, visible):
        found = []
        for head in range(heads):
            keys = jnp.concatenate([expanded[:, head * both : head * both + NOPE], tail], axis=1)
            one = lax.dot_general(query[head], keys, nt, preferred_element_type=jnp.float32)
            found.append(jnp.where(visible, one * score_scale, masked_score))
        return found

    seen_own = (jnp.broadcast_to(docs_here, (rows, rows)) == jnp.broadcast_to(doc_col, (rows, rows))) & (col_of <= row_of)
    kv_own = expand(lat_v[:, :KVL])
    own = score(kv_own, lat_all[back, :, KVL:], seen_own)

    for step in range(1, back + 1):
        @pl.when(c >= step)
        def _():
            latent_copy(step).wait_recv()

    count = back * rows
    tail_prev = lat_all[:back, :, KVL:].reshape(count, LANES)
    pick = (lax.broadcasted_iota(jnp.int32, (16, LANES), 1) == ROPE).astype(jnp.float32).astype(jnp.bfloat16)
    key_docs = lax.dot_general(pick, tail_prev, nt, preferred_element_type=jnp.float32)[0:1]
    exists = lax.broadcasted_iota(jnp.int32, (rows, count), 1) + (c - back) * rows >= 0
    seen_prev = (jnp.broadcast_to(key_docs, (rows, count)) == jnp.broadcast_to(doc_col, (rows, count))) & exists
    kv_prev = expand(lat_all[:back, :, :KVL].reshape(count, KVL))
    prev = score(kv_prev, tail_prev, seen_prev)
    for head in range(heads):
        highest = jnp.maximum(
            jnp.max(own[head], axis=1, keepdims=True), jnp.max(prev[head], axis=1, keepdims=True)
        )
        p_own = jnp.where(seen_own, jnp.exp(own[head] - highest), 0.0)
        p_prev = jnp.where(seen_prev, jnp.exp(prev[head] - highest), 0.0)
        total = jnp.sum(p_own, axis=1, keepdims=True) + jnp.sum(p_prev, axis=1, keepdims=True)
        columns = slice(head * both + NOPE, (head + 1) * both)
        mixed = jnp.dot(p_own.astype(jnp.bfloat16), kv_own[:, columns], preferred_element_type=jnp.float32)
        mixed = mixed + jnp.dot(p_prev.astype(jnp.bfloat16), kv_prev[:, columns], preferred_element_type=jnp.float32)
        att_v[:, head * VDIM : (head + 1) * VDIM] = (mixed / total).astype(jnp.bfloat16)

    def partial_of(role, k):
        if k == 0:
            pltpu.make_async_copy(wout_v.at[role], wout_v.at[role], wout_sem.at[role]).wait()
        return jnp.dot(att_v[...], wout_v[role, k], preferred_element_type=jnp.float32)

    def sums_copy(slot, landing, device):
        return pltpu.make_async_remote_copy(
            src_ref=sums_s.at[slot], dst_ref=sums_r.at[landing],
            send_sem=sums_send, recv_sem=sums_recv.at[landing],
            device_id={"head": device}, device_id_type=MESH,
        )

    def piece_copy(piece, landing, device):
        return pltpu.make_async_remote_copy(
            src_ref=enc_s.at[piece], dst_ref=enc_r.at[landing],
            send_sem=enc_send, recv_sem=enc_recv.at[landing],
            device_id={"head": device}, device_id_type=MESH,
        )

    def finish(k, out, encoded, squares):
        cols = slice(k * part, (k + 1) * part)
        attn_ref[:, cols] = out
        hidden = res_v[:, cols].astype(jnp.float32) + out.astype(jnp.float32)
        squares = squares + jnp.sum(hidden * hidden, axis=1, keepdims=True)
        scaled = (hidden * gain_v[cols][None]).astype(jnp.bfloat16)
        encoded = encoded + lax.dot_general(scaled, wenc_v[:, cols], nt, preferred_element_type=jnp.float32)
        return encoded, squares

    split = ROPE + (LANES - ROPE) // 2
    coarse_lanes = lax.broadcasted_iota(jnp.int32, (PIECE, LANES), 1) < split

    def pack(piece, encoded, squares):
        coarse = squares.astype(jnp.bfloat16).astype(jnp.float32)
        sums = jnp.where(
            coarse_lanes,
            jnp.broadcast_to(coarse, (PIECE, LANES)), jnp.broadcast_to(squares - coarse, (PIECE, LANES)),
        )
        enc_s[piece, :, KVL:] = sums.astype(jnp.bfloat16)
        enc_s[piece, :, : KVL + ROPE] = encoded.astype(jnp.bfloat16)

    def unpack(packed):
        squares = packed[:, KVL + ROPE : KVL + ROPE + 1] + packed[:, KVL + split : KVL + split + 1]
        return packed[:, : KVL + ROPE], squares

    def conclude(near_half):
        for piece in range(pieces):
            if near_half is None:
                piece_copy(piece, piece, partner).wait_recv()
            piece_copy(piece, pieces + piece, other).wait_recv()
            near = (enc_r[piece] if near_half is None else near_half[piece]).astype(jnp.float32)
            whole, square_sum = unpack(near + enc_r[pieces + piece].astype(jnp.float32))
            scale = lax.rsqrt(square_sum / (width * n_head) + epsilon)
            next_ref[piece * PIECE : (piece + 1) * PIECE, :] = (whole * scale).astype(jnp.bfloat16)

    for i in range(4, 7):
        loads[i].wait()
    nothing = jnp.zeros((rows, KVL + ROPE), jnp.float32), jnp.zeros((rows, 1), jnp.float32)

    @pl.when(at_end)
    def _():
        for slot in range(3 * chunks):
            role, k = divmod(slot, chunks)
            sums_s[slot] = partial_of(role, k).astype(jnp.bfloat16)
            sums_copy(slot, slot, partner).start()
        encoded, squares = nothing
        for k in range(chunks):
            mine = partial_of(3, k)
            sums_copy(k, k, partner).wait_recv()
            mine = mine + sums_r[k].astype(jnp.float32)
            sums_copy(k, chunks + k, partner).wait_recv()
            out = (mine + sums_r[chunks + k].astype(jnp.float32)).astype(jnp.bfloat16)
            encoded, squares = finish(k, out, encoded, squares)
        for piece in range(pieces):
            own_rows = slice(piece * PIECE, (piece + 1) * PIECE)
            pack(piece, encoded[own_rows], squares[own_rows])
            piece_copy(piece, piece, partner).start()
        conclude(None)

    @pl.when(at_mate)
    def _():
        for k in range(chunks):
            sums_s[2 * chunks + k] = partial_of(2, k).astype(jnp.bfloat16)
            sums_copy(2 * chunks + k, k, partner).start()
        pl.semaphore_wait(far_in, 1)
        for slot in range(2 * chunks):
            role, k = divmod(slot, chunks)
            mine = partial_of(role, k)
            sums_copy(slot, slot, partner).wait_recv()
            sums_s[slot] = (mine + sums_r[slot].astype(jnp.float32)).astype(jnp.bfloat16)
            if role == 0:
                sums_copy(slot, chunks + k, far_end).start()
            else:
                sums_copy(slot, 3 * chunks + k, other).start()
        encoded, squares = nothing
        for k in range(chunks):
            mine = partial_of(3, k)
            sums_copy(k, 3 * chunks + k, other).wait_recv()
            mine = mine + sums_r[3 * chunks + k].astype(jnp.float32)
            sums_copy(k, 2 * chunks + k, partner).wait_recv()
            out = (mine + sums_r[2 * chunks + k].astype(jnp.float32)).astype(jnp.bfloat16)
            encoded, squares = finish(k, out, encoded, squares)
        for piece in range(pieces):
            own_rows = slice(piece * PIECE, (piece + 1) * PIECE)
            piece_copy(piece, piece, partner).wait_recv()
            theirs, their_squares = unpack(enc_r[piece].astype(jnp.float32))
            pack(piece, encoded[own_rows] + theirs, squares[own_rows] + their_squares)
            piece_copy(piece, pieces + piece, far_end).start()
            piece_copy(piece, piece, partner).start()
        for piece in range(pieces):
            piece_copy(piece, pieces + piece, other).start()
        conclude(enc_s)

    for step in range(1, back + 1):
        @pl.when(c + step < n_ctx)
        def _():
            latent_copy(step).wait_send()
    all_sums = pltpu.make_async_copy(sums_s, sums_s, sums_send)
    all_sums.wait()
    all_pieces = pltpu.make_async_copy(enc_s, enc_s, enc_send)

    @pl.when(at_end)
    def _():
        all_pieces.wait()

    @pl.when(at_mate)
    def _():
        for _ in range(3):
            all_pieces.wait()


def write_out(attn_v, next_v, attn_hbm, next_hbm, sem):
    copies = [
        pltpu.make_async_copy(attn_v, attn_hbm, sem.at[0]),
        pltpu.make_async_copy(next_v, next_hbm, sem.at[1]),
    ]
    for copy in copies:
        copy.start()
    for copy in copies:
        copy.wait()


def fused(n_ctx, n_head, queries, kv_latent, doc_ids, w_kv, w_out, w_enc, residual, norm_gain):
    rows = queries.shape[0]
    heads = w_kv.shape[1] // (NOPE + VDIM)
    width = residual.shape[1]
    part = width // CHUNKS
    pieces = rows // PIECE
    back = min(n_ctx - 1, -(-(n_ctx * rows // 2 - 1) // rows))
    bf16, f32 = jnp.bfloat16, jnp.float32
    hbm = pl.BlockSpec(memory_space=pltpu.HBM)
    vmem = pl.BlockSpec(memory_space=pltpu.VMEM)
    dma = pltpu.SemaphoreType.DMA
    done = pl.pallas_call(
        functools.partial(kernel, n_ctx, n_head, back, CHUNKS),
        out_shape=(pltpu.VMEM((rows, width), bf16), pltpu.VMEM((rows, KVL + ROPE), bf16)),
        in_specs=[hbm] * 8,
        out_specs=(vmem, vmem),
        scratch_shapes=[
            pltpu.VMEM(queries.shape, bf16),
            pltpu.VMEM(kv_latent.shape, bf16),
            pltpu.VMEM((1, rows), jnp.int32),
            pltpu.VMEM(w_kv.shape, bf16),
            pltpu.VMEM((4, CHUNKS, w_out.shape[0], part), bf16),
            pltpu.VMEM(w_enc.shape[::-1], bf16),
            pltpu.VMEM(residual.shape, bf16),
            pltpu.VMEM((width,), f32),
            pltpu.VMEM((back + 1, rows, KVL + LANES), bf16),
            pltpu.VMEM((rows, heads * VDIM), bf16),
            pltpu.VMEM((3 * CHUNKS, rows, part), bf16),
            pltpu.VMEM((4 * CHUNKS, rows, part), bf16),
            pltpu.VMEM((pieces, PIECE, KVL + LANES), bf16),
            pltpu.VMEM((2 * pieces, PIECE, KVL + LANES), bf16),
            dma((7,)),
            dma((4,)),
            dma((back,)),
            dma((back,)),
            dma,
            dma((4 * CHUNKS,)),
            dma,
            dma((2 * pieces,)),
            pltpu.SemaphoreType.REGULAR,
        ],
        compiler_params=pltpu.CompilerParams(
            collective_id=0, has_side_effects=True, vmem_limit_bytes=VMEM_BYTES
        ),
        name="latent_layer",
    )(
        queries, kv_latent, doc_ids[None], w_kv, w_out, w_enc.T, residual, norm_gain,
    )
    return pl.pallas_call(
        write_out,
        out_shape=tuple(pltpu.HBM(one.shape, one.dtype) for one in done),
        in_specs=[vmem] * 2,
        out_specs=(hbm, hbm),
        scratch_shapes=[dma((2,))],
        name="write_out",
    )(*[pltpu.with_memory_space_constraint(one, pltpu.VMEM) for one in done])


def general(n_ctx, n_head, queries, kv_latent, doc_ids, w_kv, w_out, w_enc, residual, norm_gain):
    rows_here = queries.shape[0]
    heads_here = w_kv.shape[1] // (NOPE + VDIM)
    query_heads = queries.reshape(rows_here, heads_here, NOPE + ROPE)
    q_nope = query_heads[:, :, :NOPE]
    q_rope = query_heads[:, :, NOPE:]
    positions = lax.axis_index("ctx") * rows_here + lax.iota(jnp.int32, rows_here)
    weights = w_kv.reshape(KVL, heads_here, NOPE + VDIM)
    f32 = jnp.float32
    latents = lax.all_gather(kv_latent, "ctx", axis=0, tiled=True)
    key_docs = lax.all_gather(doc_ids, "ctx", axis=0, tiled=True)
    key_pos = lax.iota(jnp.int32, latents.shape[0])
    content = latents[:, :KVL]
    rotary = latents[:, KVL:]
    both = jnp.einsum("nc,chd->nhd", content, weights, preferred_element_type=f32).astype(jnp.bfloat16)
    keys = both[:, :, :NOPE]
    values = both[:, :, NOPE:]
    scores = jnp.einsum("qhd,nhd->hqn", q_nope, keys, preferred_element_type=f32)
    scores = scores + jnp.einsum("qhd,nd->hqn", q_rope, rotary, preferred_element_type=f32)
    visible = (key_docs[None, :] == doc_ids[:, None]) & (key_pos[None, :] <= positions[:, None])
    scores = jnp.where(visible[None], scores * (1.0 / math.sqrt(NOPE + ROPE)), masked_score)
    highest = jnp.max(scores, axis=2)
    probs = jnp.where(visible[None], jnp.exp(scores - highest[:, :, None]), 0.0)
    total = jnp.sum(probs, axis=2)
    mixed = jnp.einsum("hqn,nhd->hqd", probs.astype(jnp.bfloat16), values, preferred_element_type=f32)
    attended = (mixed / total[:, :, None]).astype(jnp.bfloat16)
    side_by_side = attended.transpose(1, 0, 2).reshape(rows_here, heads_here * VDIM)
    summed = lax.psum_scatter(
        lax.dot_general(w_out, side_by_side, (((0,), (1,)), ((), ())), preferred_element_type=f32),
        "head", scatter_dimension=0, tiled=True,
    )
    attn_out = summed.T.astype(jnp.bfloat16)
    hidden = residual.astype(f32) + attn_out.astype(f32)
    squares = jnp.sum(hidden * hidden, axis=1)
    scaled = (hidden * norm_gain[None, :]).astype(jnp.bfloat16)
    encoded = jnp.dot(scaled, w_enc, preferred_element_type=f32)
    enc_sum, sq_sum = lax.psum((encoded, squares), "head")
    next_latent = (enc_sum * lax.rsqrt(sq_sum / D + epsilon)[:, None]).astype(jnp.bfloat16)
    return (attn_out, next_latent)


def per_device(n_ctx, n_head, *args):
    rows, width = args[6].shape
    whole_tiles = width % (CHUNKS * LANES) == 0 and rows % PIECE == 0 and rows <= LANES
    body = fused if n_head == 4 and whole_tiles else general
    return body(n_ctx, n_head, *args)


def solution(mesh):
    return jax.shard_map(
        functools.partial(per_device, mesh.shape["ctx"], mesh.shape["head"]),
        mesh=mesh,
        in_specs=(
            P(("rep", "ctx"), "head"),
            P(("rep", "ctx"), None),
            P(("rep", "ctx")),
            P(None, "head"),
            P("head", None),
            P("head", None),
            P(("rep", "ctx"), "head"),
            P("head"),
        ),
        out_specs=(P(("rep", "ctx"), "head"), P(("rep", "ctx"), None)),
        check_vma=False,
    )
```

```python
import functools
import math

import jax
import jax.numpy as jnp
from jax import lax
from jax.experimental import pallas as pl
from jax.experimental.pallas import tpu as pltpu
from jax.sharding import PartitionSpec as P

D = 7168
KVL = 512
ROPE = 64
NOPE = 128
VDIM = 128

LANES = 128
CHUNKS = 7
PIECE = 16
VMEM_BYTES = 60 * 1024 * 1024
MESH = pl.DeviceIdType.MESH

masked_score = -1e30
epsilon = 1e-06


def kernel(
    n_ctx, n_head, n_rep, back, chunks,
    q_hbm, lat_hbm, doc_hbm, wkv_hbm, wout_hbm, wenc_hbm, res_hbm, gain_hbm,
    attn_ref, next_ref,
    q_v, lat_v, doc_v, wkv_v, wout_v, wenc_v, res_v, gain_v,
    lat_all, att_v, sums_s, sums_r, enc_s, enc_r,
    load_sem, wout_sem, lat_send, lat_recv, sums_send, sums_recv,
    enc_send, enc_recv, far_in, turn,
):
    rows = q_hbm.shape[0]
    heads = wkv_hbm.shape[1] // (NOPE + VDIM)
    width = res_hbm.shape[1]
    part = width // chunks
    pieces = rows // PIECE
    c = lax.axis_index("ctx")
    h = lax.axis_index("head")
    r = lax.axis_index("rep")
    side = h // 2
    end, mate = 3 * side, 1 + side
    partner = h + 1 - 2 * lax.rem(h, 2)
    other = 3 - mate
    at_end = h == end
    at_mate = h == mate
    far_end = 3 - end
    slices = (far_end, other, partner, h)

    loads = []
    for i, (src, dst) in enumerate((
        (lat_hbm, lat_v), (doc_hbm, doc_v), (q_hbm, q_v), (wkv_hbm, wkv_v),
        (res_hbm, res_v), (wenc_hbm, wenc_v), (gain_hbm, gain_v),
    )):
        loads.append(pltpu.make_async_copy(src, dst, load_sem.at[i]))
    for i in range(4):
        loads[i].start()

    barrier = pltpu.get_barrier_semaphore()
    near = [("ctx", c, step, n_ctx) for step in range(1, back + 1)] + [("head", h, 1, n_head), ("rep", r, 1, n_rep)]
    for axis, here, step, count in near:
        @pl.when(here + step < count)
        def _():
            pl.semaphore_signal(barrier, inc=1, device_id={axis: here + step}, device_id_type=MESH)

        @pl.when(here >= step)
        def _():
            pl.semaphore_signal(barrier, inc=1, device_id={axis: here - step}, device_id_type=MESH)

    wout_loads = []
    for role in range(4):
        start = pl.multiple_of(slices[role] * width, LANES)
        wout_loads.append(pltpu.make_async_copy(
            wout_hbm.at[:, pl.ds(start, width)], wout_v.at[role], wout_sem.at[role]
        ))
        wout_loads[-1].start()
    for i in range(4, 7):
        loads[i].start()

    loads[0].wait()
    loads[1].wait()
    docs_here = doc_v[...].astype(jnp.float32)
    row_of = lax.broadcasted_iota(jnp.int32, (rows, rows), 0)
    col_of = lax.broadcasted_iota(jnp.int32, (rows, rows), 1)
    doc_col = jnp.sum(
        jnp.where(row_of == col_of, jnp.broadcast_to(docs_here, (rows, rows)), 0.0), axis=1, keepdims=True
    )
    lat_all[back, :, KVL:] = jnp.broadcast_to(doc_col, (rows, LANES)).astype(jnp.bfloat16)
    lat_all[back, :, : KVL + ROPE] = lat_v[...]
    for step in range(1, back + 1):
        @pl.when(c < step)
        def _():
            lat_all[back - step] = jnp.zeros((rows, KVL + LANES), jnp.bfloat16)

    peers = 0
    for axis, here, step, count in near:
        peers = peers + (here + step < count).astype(jnp.int32) + (here >= step).astype(jnp.int32)
    pl.semaphore_wait(barrier, peers)

    @pl.when(at_mate)
    def _():
        pl.semaphore_signal(far_in, inc=1, device_id={"head": other}, device_id_type=MESH)


    def latent_copy(step):
        return pltpu.make_async_remote_copy(
            src_ref=lat_all.at[back], dst_ref=lat_all.at[back - step],
            send_sem=lat_send.at[step - 1], recv_sem=lat_recv.at[step - 1],
            device_id={"ctx": lax.rem(c + step, n_ctx)}, device_id_type=MESH,
        )

    for step in range(1, back + 1):
        @pl.when(c + step < n_ctx)
        def _():
            latent_copy(step).start()

    loads[2].wait()
    low = lax.broadcasted_iota(jnp.int32, (rows, LANES), 1) < ROPE
    query = []
    for head in range(heads):
        first, shift = divmod(head * (NOPE + ROPE), LANES)
        a = q_v[:, first * LANES : (first + 1) * LANES].astype(jnp.float32)
        b = q_v[:, (first + 1) * LANES : (first + 2) * LANES].astype(jnp.float32)
        if shift:
            a = pltpu.roll(a, shift, 1)
            b = pltpu.roll(b, shift, 1)
            a = jnp.where(low, a, b)
        query.append(jnp.concatenate([a, jnp.where(low, b, 0.0)], axis=1).astype(jnp.bfloat16))
    loads[3].wait()

    nt = (((1,), (1,)), ((), ()))
    score_scale = 1.0 / math.sqrt(NOPE + ROPE)
    both = NOPE + VDIM

    def expand(latent):
        return jnp.dot(latent, wkv_v[...], preferred_element_type=jnp.float32).astype(jnp.bfloat16)

    def score(expanded, tail, visible):
        found = []
        for head in range(heads):
            keys = jnp.concatenate([expanded[:, head * both : head * both + NOPE], tail], axis=1)
            one = lax.dot_general(query[head], keys, nt, preferred_element_type=jnp.float32)
            found.append(jnp.where(visible, one * score_scale, masked_score))
        return found

    seen_own = (jnp.broadcast_to(docs_here, (rows, rows)) == jnp.broadcast_to(doc_col, (rows, rows))) & (col_of <= row_of)
    kv_own = expand(lat_v[:, :KVL])
    own = score(kv_own, lat_all[back, :, KVL:], seen_own)


    def attend(head, weighted, total):
        att_v[:, head * VDIM : (head + 1) * VDIM] = (weighted / total).astype(jnp.bfloat16)

    def values(expanded, head):
        return expanded[:, head * both + NOPE : (head + 1) * both]

    def weigh(scores, highest, visible, expanded, head):
        probs = jnp.where(visible, jnp.exp(scores - highest), 0.0)
        weighted = jnp.dot(probs.astype(jnp.bfloat16), values(expanded, head), preferred_element_type=jnp.float32)
        return weighted, jnp.sum(probs, axis=1, keepdims=True)

    @pl.when(c == 0)
    def _():
        for head in range(heads):
            highest = jnp.max(own[head], axis=1, keepdims=True)
            attend(head, *weigh(own[head], highest, seen_own, kv_own, head))

    @pl.when(c >= 1)
    def _():
        for step in range(1, back + 1):
            @pl.when(c >= step)
            def _():
                latent_copy(step).wait_recv()

        count = back * rows
        tail_prev = lat_all[:back, :, KVL:].reshape(count, LANES)
        pick = (lax.broadcasted_iota(jnp.int32, (16, LANES), 1) == ROPE).astype(jnp.float32).astype(jnp.bfloat16)
        key_docs = lax.dot_general(pick, tail_prev, nt, preferred_element_type=jnp.float32)[0:1]
        exists = lax.broadcasted_iota(jnp.int32, (rows, count), 1) + (c - back) * rows >= 0
        seen_prev = (jnp.broadcast_to(key_docs, (rows, count)) == jnp.broadcast_to(doc_col, (rows, count))) & exists
        kv_prev = expand(lat_all[:back, :, :KVL].reshape(count, KVL))
        prev = score(kv_prev, tail_prev, seen_prev)
        for head in range(heads):
            highest = jnp.maximum(
                jnp.max(own[head], axis=1, keepdims=True), jnp.max(prev[head], axis=1, keepdims=True)
            )
            here, total_here = weigh(own[head], highest, seen_own, kv_own, head)
            earlier, total_earlier = weigh(prev[head], highest, seen_prev, kv_prev, head)
            attend(head, here + earlier, total_here + total_earlier)


    def partial_of(role, k):
        if k == 0:
            wout_loads[role].wait()
        return jnp.dot(att_v[...], wout_v[role, :, k * part : (k + 1) * part], preferred_element_type=jnp.float32)

    def sums_copy(slot, landing, device):
        return pltpu.make_async_remote_copy(
            src_ref=sums_s.at[slot], dst_ref=sums_r.at[landing],
            send_sem=sums_send, recv_sem=sums_recv.at[landing],
            device_id={"head": device}, device_id_type=MESH,
        )

    def piece_copy(piece, landing, device):
        return pltpu.make_async_remote_copy(
            src_ref=enc_s.at[piece], dst_ref=enc_r.at[landing],
            send_sem=enc_send, recv_sem=enc_recv.at[landing],
            device_id={"head": device}, device_id_type=MESH,
        )

    def finish(k, out, encoded, squares):
        if k == 0:
            for i in range(4, 7):
                loads[i].wait()
        cols = slice(k * part, (k + 1) * part)
        attn_ref[:, cols] = out
        hidden = res_v[:, cols].astype(jnp.float32) + out.astype(jnp.float32)
        squares = squares + jnp.sum(hidden * hidden, axis=1, keepdims=True)
        scaled = (hidden * gain_v[cols][None]).astype(jnp.bfloat16)
        encoded = encoded + lax.dot_general(scaled, wenc_v[:, cols], nt, preferred_element_type=jnp.float32)
        return encoded, squares

    split = ROPE + (LANES - ROPE) // 2
    coarse_lanes = lax.broadcasted_iota(jnp.int32, (PIECE, LANES), 1) < split

    def pack(piece, encoded, squares):
        coarse = squares.astype(jnp.bfloat16).astype(jnp.float32)
        sums = jnp.where(
            coarse_lanes,
            jnp.broadcast_to(coarse, (PIECE, LANES)), jnp.broadcast_to(squares - coarse, (PIECE, LANES)),
        )
        enc_s[piece, :, KVL:] = sums.astype(jnp.bfloat16)
        enc_s[piece, :, : KVL + ROPE] = encoded.astype(jnp.bfloat16)

    def unpack(packed):
        squares = packed[:, KVL + ROPE : KVL + ROPE + 1] + packed[:, KVL + split : KVL + split + 1]
        return packed[:, : KVL + ROPE], squares

    def give_turn():
        @pl.when(r + 1 < n_rep)
        def _():
            pl.semaphore_signal(turn, inc=1, device_id={"rep": r + 1}, device_id_type=MESH)

    def await_turn():
        @pl.when(r >= 1)
        def _():
            pl.semaphore_wait(turn, 1)

    def conclude(near_half):
        for piece in range(pieces):
            if near_half is None:
                piece_copy(piece, piece, partner).wait_recv()
            piece_copy(piece, pieces + piece, other).wait_recv()
            near = (enc_r[piece] if near_half is None else near_half[piece]).astype(jnp.float32)
            whole, square_sum = unpack(near + enc_r[pieces + piece].astype(jnp.float32))
            scale = lax.rsqrt(square_sum / (width * n_head) + epsilon)
            next_ref[piece * PIECE : (piece + 1) * PIECE, :] = (whole * scale).astype(jnp.bfloat16)

    nothing = jnp.zeros((rows, KVL + ROPE), jnp.float32), jnp.zeros((rows, 1), jnp.float32)

    @pl.when(at_end)
    def _():
        for slot in range(3 * chunks):
            role, k = divmod(slot, chunks)
            if slot == 2 * chunks:
                await_turn()
            sums_s[slot] = partial_of(role, k).astype(jnp.bfloat16)
            sums_copy(slot, slot, partner).start()
        encoded, squares = nothing
        for k in range(chunks):
            mine = partial_of(3, k)
            sums_copy(k, k, partner).wait_recv()
            mine = mine + sums_r[k].astype(jnp.float32)
            sums_copy(k, chunks + k, partner).wait_recv()
            if k == 0:
                give_turn()
            out = (mine + sums_r[chunks + k].astype(jnp.float32)).astype(jnp.bfloat16)
            encoded, squares = finish(k, out, encoded, squares)
        for piece in range(pieces):
            own_rows = slice(piece * PIECE, (piece + 1) * PIECE)
            pack(piece, encoded[own_rows], squares[own_rows])
            piece_copy(piece, piece, partner).start()
        conclude(None)

    @pl.when(at_mate)
    def _():
        for k in range(chunks):
            sums_s[2 * chunks + k] = partial_of(2, k).astype(jnp.bfloat16)
            sums_copy(2 * chunks + k, k, partner).start()
        pl.semaphore_wait(far_in, 1)
        for slot in range(2 * chunks):
            role, k = divmod(slot, chunks)
            mine = partial_of(role, k)
            sums_copy(slot, slot, partner).wait_recv()
            sums_s[slot] = (mine + sums_r[slot].astype(jnp.float32)).astype(jnp.bfloat16)
            if role == 0:
                sums_copy(slot, chunks + k, far_end).start()
            else:
                sums_copy(slot, 3 * chunks + k, other).start()
        encoded, squares = nothing
        for k in range(chunks):
            mine = partial_of(3, k)
            sums_copy(k, 3 * chunks + k, other).wait_recv()
            mine = mine + sums_r[3 * chunks + k].astype(jnp.float32)
            sums_copy(k, 2 * chunks + k, partner).wait_recv()
            out = (mine + sums_r[2 * chunks + k].astype(jnp.float32)).astype(jnp.bfloat16)
            encoded, squares = finish(k, out, encoded, squares)
        for piece in range(pieces):
            own_rows = slice(piece * PIECE, (piece + 1) * PIECE)
            piece_copy(piece, piece, partner).wait_recv()
            theirs, their_squares = unpack(enc_r[piece].astype(jnp.float32))
            pack(piece, encoded[own_rows] + theirs, squares[own_rows] + their_squares)
            piece_copy(piece, pieces + piece, far_end).start()
            piece_copy(piece, piece, partner).start()
        for piece in range(pieces):
            piece_copy(piece, pieces + piece, other).start()
        conclude(enc_s)

    for step in range(1, back + 1):
        @pl.when(c + step < n_ctx)
        def _():
            latent_copy(step).wait_send()
    all_sums = pltpu.make_async_copy(sums_s, sums_s, sums_send)
    all_sums.wait()
    all_pieces = pltpu.make_async_copy(enc_s, enc_s, enc_send)

    @pl.when(at_end)
    def _():
        all_pieces.wait()

    @pl.when(at_mate)
    def _():
        for _ in range(3):
            all_pieces.wait()


def write_out(attn_v, next_v, attn_hbm, next_hbm, sem):
    copies = [
        pltpu.make_async_copy(attn_v, attn_hbm, sem.at[0]),
        pltpu.make_async_copy(next_v, next_hbm, sem.at[1]),
    ]
    for copy in copies:
        copy.start()
    for copy in copies:
        copy.wait()


def fused(n_ctx, n_head, n_rep, queries, kv_latent, doc_ids, w_kv, w_out, w_enc, residual, norm_gain):
    rows = queries.shape[0]
    heads = w_kv.shape[1] // (NOPE + VDIM)
    width = residual.shape[1]
    part = width // CHUNKS
    pieces = rows // PIECE
    back = min(n_ctx - 1, -(-(n_ctx * rows // 2 - 1) // rows))
    bf16, f32 = jnp.bfloat16, jnp.float32
    hbm = pl.BlockSpec(memory_space=pltpu.HBM)
    vmem = pl.BlockSpec(memory_space=pltpu.VMEM)
    dma = pltpu.SemaphoreType.DMA
    done = pl.pallas_call(
        functools.partial(kernel, n_ctx, n_head, n_rep, back, CHUNKS),
        out_shape=(pltpu.VMEM((rows, width), bf16), pltpu.VMEM((rows, KVL + ROPE), bf16)),
        in_specs=[hbm] * 8,
        out_specs=(vmem, vmem),
        scratch_shapes=[
            pltpu.VMEM(queries.shape, bf16),
            pltpu.VMEM(kv_latent.shape, bf16),
            pltpu.VMEM((1, rows), jnp.int32),
            pltpu.VMEM(w_kv.shape, bf16),
            pltpu.VMEM((4, w_out.shape[0], width), bf16),
            pltpu.VMEM(w_enc.shape[::-1], bf16),
            pltpu.VMEM(residual.shape, bf16),
            pltpu.VMEM((width,), f32),
            pltpu.VMEM((back + 1, rows, KVL + LANES), bf16),
            pltpu.VMEM((rows, heads * VDIM), bf16),
            pltpu.VMEM((3 * CHUNKS, rows, part), bf16),
            pltpu.VMEM((4 * CHUNKS, rows, part), bf16),
            pltpu.VMEM((pieces, PIECE, KVL + LANES), bf16),
            pltpu.VMEM((2 * pieces, PIECE, KVL + LANES), bf16),
            dma((7,)),
            dma((4,)),
            dma((back,)),
            dma((back,)),
            dma,
            dma((4 * CHUNKS,)),
            dma,
            dma((2 * pieces,)),
            pltpu.SemaphoreType.REGULAR,
            pltpu.SemaphoreType.REGULAR,
        ],
        compiler_params=pltpu.CompilerParams(
            collective_id=0, has_side_effects=True, vmem_limit_bytes=VMEM_BYTES
        ),
        name="latent_layer",
    )(
        queries, kv_latent, doc_ids[None], w_kv, w_out, w_enc.T, residual, norm_gain,
    )
    return pl.pallas_call(
        write_out,
        out_shape=tuple(pltpu.HBM(one.shape, one.dtype) for one in done),
        in_specs=[vmem] * 2,
        out_specs=(hbm, hbm),
        scratch_shapes=[dma((2,))],
        name="write_out",
    )(*[pltpu.with_memory_space_constraint(one, pltpu.VMEM) for one in done])


def general(n_ctx, n_head, n_rep, queries, kv_latent, doc_ids, w_kv, w_out, w_enc, residual, norm_gain):
    rows_here = queries.shape[0]
    heads_here = w_kv.shape[1] // (NOPE + VDIM)
    query_heads = queries.reshape(rows_here, heads_here, NOPE + ROPE)
    q_nope = query_heads[:, :, :NOPE]
    q_rope = query_heads[:, :, NOPE:]
    positions = lax.axis_index("ctx") * rows_here + lax.iota(jnp.int32, rows_here)
    weights = w_kv.reshape(KVL, heads_here, NOPE + VDIM)
    f32 = jnp.float32
    latents = lax.all_gather(kv_latent, "ctx", axis=0, tiled=True)
    key_docs = lax.all_gather(doc_ids, "ctx", axis=0, tiled=True)
    key_pos = lax.iota(jnp.int32, latents.shape[0])
    content = latents[:, :KVL]
    rotary = latents[:, KVL:]
    both = jnp.einsum("nc,chd->nhd", content, weights, preferred_element_type=f32).astype(jnp.bfloat16)
    keys = both[:, :, :NOPE]
    values = both[:, :, NOPE:]
    scores = jnp.einsum("qhd,nhd->hqn", q_nope, keys, preferred_element_type=f32)
    scores = scores + jnp.einsum("qhd,nd->hqn", q_rope, rotary, preferred_element_type=f32)
    visible = (key_docs[None, :] == doc_ids[:, None]) & (key_pos[None, :] <= positions[:, None])
    scores = jnp.where(visible[None], scores * (1.0 / math.sqrt(NOPE + ROPE)), masked_score)
    highest = jnp.max(scores, axis=2)
    probs = jnp.where(visible[None], jnp.exp(scores - highest[:, :, None]), 0.0)
    total = jnp.sum(probs, axis=2)
    mixed = jnp.einsum("hqn,nhd->hqd", probs.astype(jnp.bfloat16), values, preferred_element_type=f32)
    attended = (mixed / total[:, :, None]).astype(jnp.bfloat16)
    side_by_side = attended.transpose(1, 0, 2).reshape(rows_here, heads_here * VDIM)
    summed = lax.psum_scatter(
        lax.dot_general(w_out, side_by_side, (((0,), (1,)), ((), ())), preferred_element_type=f32),
        "head", scatter_dimension=0, tiled=True,
    )
    attn_out = summed.T.astype(jnp.bfloat16)
    hidden = residual.astype(f32) + attn_out.astype(f32)
    squares = jnp.sum(hidden * hidden, axis=1)
    scaled = (hidden * norm_gain[None, :]).astype(jnp.bfloat16)
    encoded = jnp.dot(scaled, w_enc, preferred_element_type=f32)
    enc_sum, sq_sum = lax.psum((encoded, squares), "head")
    next_latent = (enc_sum * lax.rsqrt(sq_sum / D + epsilon)[:, None]).astype(jnp.bfloat16)
    return (attn_out, next_latent)


def per_device(n_ctx, n_head, n_rep, *args):
    rows, width = args[6].shape
    whole_tiles = width % (CHUNKS * LANES) == 0 and rows % PIECE == 0 and rows <= LANES
    line = n_head == 4 and n_rep == 2
    body = fused if line and whole_tiles else general
    return body(n_ctx, n_head, n_rep, *args)


def solution(mesh):
    return jax.shard_map(
        functools.partial(per_device, mesh.shape["ctx"], mesh.shape["head"], mesh.shape["rep"]),
        mesh=mesh,
        in_specs=(
            P(("rep", "ctx"), "head"),
            P(("rep", "ctx"), None),
            P(("rep", "ctx")),
            P(None, "head"),
            P("head", None),
            P("head", None),
            P(("rep", "ctx"), "head"),
            P("head"),
        ),
        out_specs=(P(("rep", "ctx"), "head"), P(("rep", "ctx"), None)),
        check_vma=False,
    )
```

```python
import functools
import math

import jax
import jax.numpy as jnp
from jax import lax
from jax.experimental import pallas as pl
from jax.experimental.pallas import tpu as pltpu
from jax.sharding import PartitionSpec as P

D = 7168
KVL = 512
ROPE = 64
NOPE = 128
VDIM = 128

LANES = 128
CHUNKS = 7
PIECE = 16
VMEM_BYTES = 60 * 1024 * 1024
MESH = pl.DeviceIdType.MESH

masked_score = -1e30
epsilon = 1e-06


def kernel(
    n_ctx, n_head, n_rep, back, chunks,
    q_hbm, lat_hbm, doc_hbm, wkv_hbm, wout_hbm, wenc_hbm, res_hbm, gain_hbm,
    attn_ref, next_ref,
    q_v, lat_v, doc_v, wkv_v, wout_v, wenc_v, res_v, gain_v,
    lat_all, att_v, sums_s, sums_r, enc_s, enc_r,
    load_sem, wout_sem, lat_send, lat_recv, sums_send, sums_recv,
    enc_send, enc_recv, far_in, turn,
):
    rows = q_hbm.shape[0]
    heads = wkv_hbm.shape[1] // (NOPE + VDIM)
    width = res_hbm.shape[1]
    part = width // chunks
    pieces = rows // PIECE
    c = lax.axis_index("ctx")
    h = lax.axis_index("head")
    r = lax.axis_index("rep")
    side = h // 2
    end, mate = 3 * side, 1 + side
    partner = h + 1 - 2 * lax.rem(h, 2)
    other = 3 - mate
    at_end = h == end
    at_mate = h == mate
    far_end = 3 - end
    slices = (far_end, other, partner, h)

    loads = []
    for i, (src, dst) in enumerate((
        (lat_hbm, lat_v), (doc_hbm, doc_v), (q_hbm, q_v), (wkv_hbm, wkv_v),
        (res_hbm, res_v), (wenc_hbm, wenc_v), (gain_hbm, gain_v),
    )):
        loads.append(pltpu.make_async_copy(src, dst, load_sem.at[i]))
    for i in range(4):
        loads[i].start()

    barrier = pltpu.get_barrier_semaphore()
    near = [("ctx", c, step, n_ctx) for step in range(1, back + 1)] + [("head", h, 1, n_head), ("rep", r, 1, n_rep)]
    for axis, here, step, count in near:
        @pl.when(here + step < count)
        def _():
            pl.semaphore_signal(barrier, inc=1, device_id={axis: here + step}, device_id_type=MESH)

        @pl.when(here >= step)
        def _():
            pl.semaphore_signal(barrier, inc=1, device_id={axis: here - step}, device_id_type=MESH)

    wout_loads = []
    for role in range(4):
        start = pl.multiple_of(slices[role] * width, LANES)
        wout_loads.append(pltpu.make_async_copy(
            wout_hbm.at[:, pl.ds(start, width)], wout_v.at[role], wout_sem.at[role]
        ))
        wout_loads[-1].start()
    for i in range(4, 7):
        loads[i].start()

    loads[0].wait()
    loads[1].wait()
    docs_here = doc_v[...].astype(jnp.float32)
    row_of = lax.broadcasted_iota(jnp.int32, (rows, rows), 0)
    col_of = lax.broadcasted_iota(jnp.int32, (rows, rows), 1)
    doc_col = jnp.sum(
        jnp.where(row_of == col_of, jnp.broadcast_to(docs_here, (rows, rows)), 0.0), axis=1, keepdims=True
    )
    lat_all[back, :, KVL:] = jnp.broadcast_to(doc_col, (rows, LANES)).astype(jnp.bfloat16)
    lat_all[back, :, : KVL + ROPE] = lat_v[...]
    for step in range(1, back + 1):
        @pl.when(c < step)
        def _():
            lat_all[back - step] = jnp.zeros((rows, KVL + LANES), jnp.bfloat16)

    peers = 0
    for axis, here, step, count in near:
        peers = peers + (here + step < count).astype(jnp.int32) + (here >= step).astype(jnp.int32)
    pl.semaphore_wait(barrier, peers)

    @pl.when(at_mate)
    def _():
        pl.semaphore_signal(far_in, inc=1, device_id={"head": other}, device_id_type=MESH)


    def latent_copy(step):
        return pltpu.make_async_remote_copy(
            src_ref=lat_all.at[back], dst_ref=lat_all.at[back - step],
            send_sem=lat_send.at[step - 1], recv_sem=lat_recv.at[step - 1],
            device_id={"ctx": lax.rem(c + step, n_ctx)}, device_id_type=MESH,
        )

    for step in range(1, back + 1):
        @pl.when(c + step < n_ctx)
        def _():
            latent_copy(step).start()

    loads[2].wait()
    low = lax.broadcasted_iota(jnp.int32, (rows, LANES), 1) < ROPE
    query = []
    for head in range(heads):
        first, shift = divmod(head * (NOPE + ROPE), LANES)
        a = q_v[:, first * LANES : (first + 1) * LANES].astype(jnp.float32)
        b = q_v[:, (first + 1) * LANES : (first + 2) * LANES].astype(jnp.float32)
        if shift:
            a = pltpu.roll(a, shift, 1)
            b = pltpu.roll(b, shift, 1)
            a = jnp.where(low, a, b)
        query.append(jnp.concatenate([a, jnp.where(low, b, 0.0)], axis=1).astype(jnp.bfloat16))
    loads[3].wait()

    nt = (((1,), (1,)), ((), ()))
    score_scale = 1.0 / math.sqrt(NOPE + ROPE)
    both = NOPE + VDIM

    def expand(latent):
        return jnp.dot(latent, wkv_v[...], preferred_element_type=jnp.float32).astype(jnp.bfloat16)

    def score(expanded, tail, visible):
        found = []
        for head in range(heads):
            keys = jnp.concatenate([expanded[:, head * both : head * both + NOPE], tail], axis=1)
            one = lax.dot_general(query[head], keys, nt, preferred_element_type=jnp.float32)
            found.append(jnp.where(visible, one * score_scale, masked_score))
        return found

    seen_own = (jnp.broadcast_to(docs_here, (rows, rows)) == jnp.broadcast_to(doc_col, (rows, rows))) & (col_of <= row_of)
    kv_own = expand(lat_v[:, :KVL])
    own = score(kv_own, lat_all[back, :, KVL:], seen_own)


    def attend(head, weighted, total):
        att_v[:, head * VDIM : (head + 1) * VDIM] = (weighted / total).astype(jnp.bfloat16)

    def values(expanded, head):
        return expanded[:, head * both + NOPE : (head + 1) * both]

    def weigh(scores, highest, visible, expanded, head):
        probs = jnp.where(visible, jnp.exp(scores - highest), 0.0)
        weighted = jnp.dot(probs.astype(jnp.bfloat16), values(expanded, head), preferred_element_type=jnp.float32)
        return weighted, jnp.sum(probs, axis=1, keepdims=True)

    @pl.when(c == 0)
    def _():
        for head in range(heads):
            highest = jnp.max(own[head], axis=1, keepdims=True)
            attend(head, *weigh(own[head], highest, seen_own, kv_own, head))

    @pl.when(c >= 1)
    def _():
        for step in range(1, back + 1):
            @pl.when(c >= step)
            def _():
                latent_copy(step).wait_recv()

        count = back * rows
        tail_prev = lat_all[:back, :, KVL:].reshape(count, LANES)
        pick = (lax.broadcasted_iota(jnp.int32, (16, LANES), 1) == ROPE).astype(jnp.float32).astype(jnp.bfloat16)
        key_docs = lax.dot_general(pick, tail_prev, nt, preferred_element_type=jnp.float32)[0:1]
        exists = lax.broadcasted_iota(jnp.int32, (rows, count), 1) + (c - back) * rows >= 0
        seen_prev = (jnp.broadcast_to(key_docs, (rows, count)) == jnp.broadcast_to(doc_col, (rows, count))) & exists
        kv_prev = expand(lat_all[:back, :, :KVL].reshape(count, KVL))
        prev = score(kv_prev, tail_prev, seen_prev)
        for head in range(heads):
            highest = jnp.maximum(
                jnp.max(own[head], axis=1, keepdims=True), jnp.max(prev[head], axis=1, keepdims=True)
            )
            here, total_here = weigh(own[head], highest, seen_own, kv_own, head)
            earlier, total_earlier = weigh(prev[head], highest, seen_prev, kv_prev, head)
            attend(head, here + earlier, total_here + total_earlier)


    def partial_of(role, k):
        if k == 0:
            wout_loads[role].wait()
        return jnp.dot(att_v[...], wout_v[role, :, k * part : (k + 1) * part], preferred_element_type=jnp.float32)

    early = 2 * chunks

    def sums_copy(slot, landing, device):
        return pltpu.make_async_remote_copy(
            src_ref=sums_s.at[slot], dst_ref=sums_r.at[landing],
            send_sem=sums_send.at[0 if slot < early else 1], recv_sem=sums_recv.at[landing],
            device_id={"head": device}, device_id_type=MESH,
        )

    def piece_copy(piece, landing, device):
        return pltpu.make_async_remote_copy(
            src_ref=enc_s.at[piece], dst_ref=enc_r.at[landing],
            send_sem=enc_send, recv_sem=enc_recv.at[landing],
            device_id={"head": device}, device_id_type=MESH,
        )

    def finish(k, out, encoded, squares):
        if k == 0:
            for i in range(4, 7):
                loads[i].wait()
        cols = slice(k * part, (k + 1) * part)
        attn_ref[:, cols] = out
        hidden = res_v[:, cols].astype(jnp.float32) + out.astype(jnp.float32)
        squares = squares + jnp.sum(hidden * hidden, axis=1, keepdims=True)
        scaled = (hidden * gain_v[cols][None]).astype(jnp.bfloat16)
        encoded = encoded + lax.dot_general(scaled, wenc_v[:, cols], nt, preferred_element_type=jnp.float32)
        return encoded, squares

    split = ROPE + (LANES - ROPE) // 2
    coarse_lanes = lax.broadcasted_iota(jnp.int32, (PIECE, LANES), 1) < split

    def pack(piece, encoded, squares):
        coarse = squares.astype(jnp.bfloat16).astype(jnp.float32)
        sums = jnp.where(
            coarse_lanes,
            jnp.broadcast_to(coarse, (PIECE, LANES)), jnp.broadcast_to(squares - coarse, (PIECE, LANES)),
        )
        enc_s[piece, :, KVL:] = sums.astype(jnp.bfloat16)
        enc_s[piece, :, : KVL + ROPE] = encoded.astype(jnp.bfloat16)

    def unpack(packed):
        squares = packed[:, KVL + ROPE : KVL + ROPE + 1] + packed[:, KVL + split : KVL + split + 1]
        return packed[:, : KVL + ROPE], squares

    def sent(buffer, sem):
        pltpu.make_async_copy(buffer, buffer, sem).wait()

    def give_turn():
        @pl.when(r + 1 < n_rep)
        def _():
            sent(sums_s.at[:early], sums_send.at[0])
            pl.semaphore_signal(turn, inc=1, device_id={"rep": r + 1}, device_id_type=MESH)

    def await_turn():
        @pl.when(r >= 1)
        def _():
            pl.semaphore_wait(turn, 1)

    def conclude(near_half):
        for piece in range(pieces):
            if near_half is None:
                piece_copy(piece, piece, partner).wait_recv()
            piece_copy(piece, pieces + piece, other).wait_recv()
            near = (enc_r[piece] if near_half is None else near_half[piece]).astype(jnp.float32)
            whole, square_sum = unpack(near + enc_r[pieces + piece].astype(jnp.float32))
            scale = lax.rsqrt(square_sum / (width * n_head) + epsilon)
            next_ref[piece * PIECE : (piece + 1) * PIECE, :] = (whole * scale).astype(jnp.bfloat16)

    nothing = jnp.zeros((rows, KVL + ROPE), jnp.float32), jnp.zeros((rows, 1), jnp.float32)

    @pl.when(at_end)
    def _():
        for slot in range(3 * chunks):
            role, k = divmod(slot, chunks)
            if slot == chunks + 4:
                await_turn()
            sums_s[slot] = partial_of(role, k).astype(jnp.bfloat16)
            sums_copy(slot, slot, partner).start()
        give_turn()
        encoded, squares = nothing
        for k in range(chunks):
            mine = partial_of(3, k)
            sums_copy(k, k, partner).wait_recv()
            mine = mine + sums_r[k].astype(jnp.float32)
            sums_copy(k, chunks + k, partner).wait_recv()
            out = (mine + sums_r[chunks + k].astype(jnp.float32)).astype(jnp.bfloat16)
            encoded, squares = finish(k, out, encoded, squares)
        for piece in range(pieces):
            own_rows = slice(piece * PIECE, (piece + 1) * PIECE)
            pack(piece, encoded[own_rows], squares[own_rows])
            piece_copy(piece, piece, partner).start()
        conclude(None)

    @pl.when(at_mate)
    def _():
        for k in range(chunks):
            sums_s[2 * chunks + k] = partial_of(2, k).astype(jnp.bfloat16)
            sums_copy(2 * chunks + k, k, partner).start()
        pl.semaphore_wait(far_in, 1)
        for slot in range(2 * chunks):
            role, k = divmod(slot, chunks)
            mine = partial_of(role, k)
            sums_copy(slot, slot, partner).wait_recv()
            sums_s[slot] = (mine + sums_r[slot].astype(jnp.float32)).astype(jnp.bfloat16)
            if role == 0:
                sums_copy(slot, chunks + k, far_end).start()
            else:
                sums_copy(slot, 3 * chunks + k, other).start()
        encoded, squares = nothing
        for k in range(chunks):
            mine = partial_of(3, k)
            sums_copy(k, 3 * chunks + k, other).wait_recv()
            mine = mine + sums_r[3 * chunks + k].astype(jnp.float32)
            sums_copy(k, 2 * chunks + k, partner).wait_recv()
            out = (mine + sums_r[2 * chunks + k].astype(jnp.float32)).astype(jnp.bfloat16)
            encoded, squares = finish(k, out, encoded, squares)
        for piece in range(pieces):
            own_rows = slice(piece * PIECE, (piece + 1) * PIECE)
            piece_copy(piece, piece, partner).wait_recv()
            theirs, their_squares = unpack(enc_r[piece].astype(jnp.float32))
            pack(piece, encoded[own_rows] + theirs, squares[own_rows] + their_squares)
            piece_copy(piece, pieces + piece, far_end).start()
            piece_copy(piece, piece, partner).start()
        for piece in range(pieces):
            piece_copy(piece, pieces + piece, other).start()
        conclude(enc_s)

    for step in range(1, back + 1):
        @pl.when(c + step < n_ctx)
        def _():
            latent_copy(step).wait_send()
    @pl.when(at_mate | (r + 1 == n_rep))
    def _():
        sent(sums_s.at[:early], sums_send.at[0])

    sent(sums_s.at[early:], sums_send.at[1])
    all_pieces = pltpu.make_async_copy(enc_s, enc_s, enc_send)

    @pl.when(at_end)
    def _():
        all_pieces.wait()

    @pl.when(at_mate)
    def _():
        for _ in range(3):
            all_pieces.wait()


def write_out(attn_v, next_v, attn_hbm, next_hbm, sem):
    copies = [
        pltpu.make_async_copy(attn_v, attn_hbm, sem.at[0]),
        pltpu.make_async_copy(next_v, next_hbm, sem.at[1]),
    ]
    for copy in copies:
        copy.start()
    for copy in copies:
        copy.wait()


def fused(n_ctx, n_head, n_rep, queries, kv_latent, doc_ids, w_kv, w_out, w_enc, residual, norm_gain):
    rows = queries.shape[0]
    heads = w_kv.shape[1] // (NOPE + VDIM)
    width = residual.shape[1]
    part = width // CHUNKS
    pieces = rows // PIECE
    back = min(n_ctx - 1, -(-(n_ctx * rows // 2 - 1) // rows))
    bf16, f32 = jnp.bfloat16, jnp.float32
    hbm = pl.BlockSpec(memory_space=pltpu.HBM)
    vmem = pl.BlockSpec(memory_space=pltpu.VMEM)
    dma = pltpu.SemaphoreType.DMA
    done = pl.pallas_call(
        functools.partial(kernel, n_ctx, n_head, n_rep, back, CHUNKS),
        out_shape=(pltpu.VMEM((rows, width), bf16), pltpu.VMEM((rows, KVL + ROPE), bf16)),
        in_specs=[hbm] * 8,
        out_specs=(vmem, vmem),
        scratch_shapes=[
            pltpu.VMEM(queries.shape, bf16),
            pltpu.VMEM(kv_latent.shape, bf16),
            pltpu.VMEM((1, rows), jnp.int32),
            pltpu.VMEM(w_kv.shape, bf16),
            pltpu.VMEM((4, w_out.shape[0], width), bf16),
            pltpu.VMEM(w_enc.shape[::-1], bf16),
            pltpu.VMEM(residual.shape, bf16),
            pltpu.VMEM((width,), f32),
            pltpu.VMEM((back + 1, rows, KVL + LANES), bf16),
            pltpu.VMEM((rows, heads * VDIM), bf16),
            pltpu.VMEM((3 * CHUNKS, rows, part), bf16),
            pltpu.VMEM((4 * CHUNKS, rows, part), bf16),
            pltpu.VMEM((pieces, PIECE, KVL + LANES), bf16),
            pltpu.VMEM((2 * pieces, PIECE, KVL + LANES), bf16),
            dma((7,)),
            dma((4,)),
            dma((back,)),
            dma((back,)),
            dma((2,)),
            dma((4 * CHUNKS,)),
            dma,
            dma((2 * pieces,)),
            pltpu.SemaphoreType.REGULAR,
            pltpu.SemaphoreType.REGULAR,
        ],
        compiler_params=pltpu.CompilerParams(
            collective_id=0, has_side_effects=True, vmem_limit_bytes=VMEM_BYTES
        ),
        name="latent_layer",
    )(
        queries, kv_latent, doc_ids[None], w_kv, w_out, w_enc.T, residual, norm_gain,
    )
    return pl.pallas_call(
        write_out,
        out_shape=tuple(pltpu.HBM(one.shape, one.dtype) for one in done),
        in_specs=[vmem] * 2,
        out_specs=(hbm, hbm),
        scratch_shapes=[dma((2,))],
        name="write_out",
    )(*[pltpu.with_memory_space_constraint(one, pltpu.VMEM) for one in done])


def general(n_ctx, n_head, n_rep, queries, kv_latent, doc_ids, w_kv, w_out, w_enc, residual, norm_gain):
    rows_here = queries.shape[0]
    heads_here = w_kv.shape[1] // (NOPE + VDIM)
    query_heads = queries.reshape(rows_here, heads_here, NOPE + ROPE)
    q_nope = query_heads[:, :, :NOPE]
    q_rope = query_heads[:, :, NOPE:]
    positions = lax.axis_index("ctx") * rows_here + lax.iota(jnp.int32, rows_here)
    weights = w_kv.reshape(KVL, heads_here, NOPE + VDIM)
    f32 = jnp.float32
    latents = lax.all_gather(kv_latent, "ctx", axis=0, tiled=True)
    key_docs = lax.all_gather(doc_ids, "ctx", axis=0, tiled=True)
    key_pos = lax.iota(jnp.int32, latents.shape[0])
    content = latents[:, :KVL]
    rotary = latents[:, KVL:]
    both = jnp.einsum("nc,chd->nhd", content, weights, preferred_element_type=f32).astype(jnp.bfloat16)
    keys = both[:, :, :NOPE]
    values = both[:, :, NOPE:]
    scores = jnp.einsum("qhd,nhd->hqn", q_nope, keys, preferred_element_type=f32)
    scores = scores + jnp.einsum("qhd,nd->hqn", q_rope, rotary, preferred_element_type=f32)
    visible = (key_docs[None, :] == doc_ids[:, None]) & (key_pos[None, :] <= positions[:, None])
    scores = jnp.where(visible[None], scores * (1.0 / math.sqrt(NOPE + ROPE)), masked_score)
    highest = jnp.max(scores, axis=2)
    probs = jnp.where(visible[None], jnp.exp(scores - highest[:, :, None]), 0.0)
    total = jnp.sum(probs, axis=2)
    mixed = jnp.einsum("hqn,nhd->hqd", probs.astype(jnp.bfloat16), values, preferred_element_type=f32)
    attended = (mixed / total[:, :, None]).astype(jnp.bfloat16)
    side_by_side = attended.transpose(1, 0, 2).reshape(rows_here, heads_here * VDIM)
    summed = lax.psum_scatter(
        lax.dot_general(w_out, side_by_side, (((0,), (1,)), ((), ())), preferred_element_type=f32),
        "head", scatter_dimension=0, tiled=True,
    )
    attn_out = summed.T.astype(jnp.bfloat16)
    hidden = residual.astype(f32) + attn_out.astype(f32)
    squares = jnp.sum(hidden * hidden, axis=1)
    scaled = (hidden * norm_gain[None, :]).astype(jnp.bfloat16)
    encoded = jnp.dot(scaled, w_enc, preferred_element_type=f32)
    enc_sum, sq_sum = lax.psum((encoded, squares), "head")
    next_latent = (enc_sum * lax.rsqrt(sq_sum / D + epsilon)[:, None]).astype(jnp.bfloat16)
    return (attn_out, next_latent)


def per_device(n_ctx, n_head, n_rep, *args):
    rows, width = args[6].shape
    whole_tiles = width % (CHUNKS * LANES) == 0 and rows % PIECE == 0 and rows <= LANES
    line = n_head == 4 and n_rep == 2
    body = fused if line and whole_tiles else general
    return body(n_ctx, n_head, n_rep, *args)


def solution(mesh):
    return jax.shard_map(
        functools.partial(per_device, mesh.shape["ctx"], mesh.shape["head"], mesh.shape["rep"]),
        mesh=mesh,
        in_specs=(
            P(("rep", "ctx"), "head"),
            P(("rep", "ctx"), None),
            P(("rep", "ctx")),
            P(None, "head"),
            P("head", None),
            P("head", None),
            P(("rep", "ctx"), "head"),
            P("head"),
        ),
        out_specs=(P(("rep", "ctx"), "head"), P(("rep", "ctx"), None)),
        check_vma=False,
    )
```

```python
import functools
import math

import jax
import jax.numpy as jnp
from jax import lax
from jax.experimental import pallas as pl
from jax.experimental.pallas import tpu as pltpu
from jax.sharding import PartitionSpec as P

D = 7168
KVL = 512
ROPE = 64
NOPE = 128
VDIM = 128

LANES = 128
CHUNKS = 7
PIECE = 16
VMEM_BYTES = 60 * 1024 * 1024
MESH = pl.DeviceIdType.MESH

masked_score = -1e30
epsilon = 1e-06


def kernel(
    n_ctx, n_head, n_rep, back, chunks,
    q_hbm, lat_hbm, doc_hbm, wkv_hbm, wout_hbm, wenc_hbm, res_hbm, gain_hbm,
    attn_ref, next_ref,
    q_v, lat_v, doc_v, wkv_v, wout_v, wenc_v, res_v, gain_v,
    lat_all, att_v, sums_s, sums_r, enc_s, enc_r,
    load_sem, wout_sem, lat_send, lat_recv, sums_send, sums_recv,
    enc_send, enc_recv, far_in, turn,
):
    rows = q_hbm.shape[0]
    heads = wkv_hbm.shape[1] // (NOPE + VDIM)
    width = res_hbm.shape[1]
    part = width // chunks
    pieces = rows // PIECE
    c = lax.axis_index("ctx")
    h = lax.axis_index("head")
    r = lax.axis_index("rep")
    side = h // 2
    end, mate = 3 * side, 1 + side
    partner = h + 1 - 2 * lax.rem(h, 2)
    other = 3 - mate
    at_end = h == end
    at_mate = h == mate
    far_end = 3 - end
    slices = (far_end, other, partner, h)

    loads = []
    for i, (src, dst) in enumerate((
        (lat_hbm, lat_v), (doc_hbm, doc_v), (q_hbm, q_v), (wkv_hbm, wkv_v),
        (res_hbm, res_v), (wenc_hbm, wenc_v), (gain_hbm, gain_v),
    )):
        loads.append(pltpu.make_async_copy(src, dst, load_sem.at[i]))
    for i in range(4):
        loads[i].start()

    barrier = pltpu.get_barrier_semaphore()
    near = [("ctx", c, step, n_ctx) for step in range(1, back + 1)] + [("head", h, 1, n_head), ("rep", r, 1, n_rep)]
    for axis, here, step, count in near:
        @pl.when(here + step < count)
        def _():
            pl.semaphore_signal(barrier, inc=1, device_id={axis: here + step}, device_id_type=MESH)

        @pl.when(here >= step)
        def _():
            pl.semaphore_signal(barrier, inc=1, device_id={axis: here - step}, device_id_type=MESH)

    wout_loads = []
    for role in range(4):
        start = pl.multiple_of(slices[role] * width, LANES)
        wout_loads.append(pltpu.make_async_copy(
            wout_hbm.at[:, pl.ds(start, width)], wout_v.at[role], wout_sem.at[role]
        ))
        wout_loads[-1].start()
    for i in range(4, 7):
        loads[i].start()

    loads[0].wait()
    loads[1].wait()
    docs_here = doc_v[...].astype(jnp.float32)
    row_of = lax.broadcasted_iota(jnp.int32, (rows, rows), 0)
    col_of = lax.broadcasted_iota(jnp.int32, (rows, rows), 1)
    doc_col = jnp.sum(
        jnp.where(row_of == col_of, jnp.broadcast_to(docs_here, (rows, rows)), 0.0), axis=1, keepdims=True
    )
    lat_all[back, :, KVL:] = jnp.broadcast_to(doc_col, (rows, LANES)).astype(jnp.bfloat16)
    lat_all[back, :, : KVL + ROPE] = lat_v[...]
    for step in range(1, back + 1):
        @pl.when(c < step)
        def _():
            lat_all[back - step] = jnp.zeros((rows, KVL + LANES), jnp.bfloat16)

    peers = 0
    for axis, here, step, count in near:
        peers = peers + (here + step < count).astype(jnp.int32) + (here >= step).astype(jnp.int32)
    pl.semaphore_wait(barrier, peers)

    @pl.when(at_mate)
    def _():
        pl.semaphore_signal(far_in, inc=1, device_id={"head": other}, device_id_type=MESH)


    def latent_copy(step):
        return pltpu.make_async_remote_copy(
            src_ref=lat_all.at[back], dst_ref=lat_all.at[back - step],
            send_sem=lat_send.at[step - 1], recv_sem=lat_recv.at[step - 1],
            device_id={"ctx": lax.rem(c + step, n_ctx)}, device_id_type=MESH,
        )

    for step in range(1, back + 1):
        @pl.when(c + step < n_ctx)
        def _():
            latent_copy(step).start()

    loads[2].wait()
    low = lax.broadcasted_iota(jnp.int32, (rows, LANES), 1) < ROPE
    query = []
    for head in range(heads):
        first, shift = divmod(head * (NOPE + ROPE), LANES)
        a = q_v[:, first * LANES : (first + 1) * LANES].astype(jnp.float32)
        b = q_v[:, (first + 1) * LANES : (first + 2) * LANES].astype(jnp.float32)
        if shift:
            a = pltpu.roll(a, shift, 1)
            b = pltpu.roll(b, shift, 1)
            a = jnp.where(low, a, b)
        query.append(jnp.concatenate([a, jnp.where(low, b, 0.0)], axis=1).astype(jnp.bfloat16))
    loads[3].wait()

    nt = (((1,), (1,)), ((), ()))
    score_scale = 1.0 / math.sqrt(NOPE + ROPE)
    both = NOPE + VDIM

    def expand(latent):
        return jnp.dot(latent, wkv_v[...], preferred_element_type=jnp.float32).astype(jnp.bfloat16)

    def score(expanded, tail, visible):
        found = []
        for head in range(heads):
            keys = jnp.concatenate([expanded[:, head * both : head * both + NOPE], tail], axis=1)
            one = lax.dot_general(query[head], keys, nt, preferred_element_type=jnp.float32)
            found.append(jnp.where(visible, one * score_scale, masked_score))
        return found

    seen_own = (jnp.broadcast_to(docs_here, (rows, rows)) == jnp.broadcast_to(doc_col, (rows, rows))) & (col_of <= row_of)
    kv_own = expand(lat_v[:, :KVL])
    own = score(kv_own, lat_all[back, :, KVL:], seen_own)


    def attend(head, weighted, total):
        att_v[:, head * VDIM : (head + 1) * VDIM] = (weighted / total).astype(jnp.bfloat16)

    def values(expanded, head):
        return expanded[:, head * both + NOPE : (head + 1) * both]

    def weigh(scores, highest, visible, expanded, head):
        probs = jnp.where(visible, jnp.exp(scores - highest), 0.0)
        weighted = jnp.dot(probs.astype(jnp.bfloat16), values(expanded, head), preferred_element_type=jnp.float32)
        return weighted, jnp.sum(probs, axis=1, keepdims=True)

    @pl.when(c == 0)
    def _():
        for head in range(heads):
            highest = jnp.max(own[head], axis=1, keepdims=True)
            attend(head, *weigh(own[head], highest, seen_own, kv_own, head))

    @pl.when(c >= 1)
    def _():
        for step in range(1, back + 1):
            @pl.when(c >= step)
            def _():
                latent_copy(step).wait_recv()

        count = back * rows
        tail_prev = lat_all[:back, :, KVL:].reshape(count, LANES)
        pick = (lax.broadcasted_iota(jnp.int32, (16, LANES), 1) == ROPE).astype(jnp.float32).astype(jnp.bfloat16)
        key_docs = lax.dot_general(pick, tail_prev, nt, preferred_element_type=jnp.float32)[0:1]
        exists = lax.broadcasted_iota(jnp.int32, (rows, count), 1) + (c - back) * rows >= 0
        seen_prev = (jnp.broadcast_to(key_docs, (rows, count)) == jnp.broadcast_to(doc_col, (rows, count))) & exists
        kv_prev = expand(lat_all[:back, :, :KVL].reshape(count, KVL))
        prev = score(kv_prev, tail_prev, seen_prev)
        for head in range(heads):
            highest = jnp.maximum(
                jnp.max(own[head], axis=1, keepdims=True), jnp.max(prev[head], axis=1, keepdims=True)
            )
            here, total_here = weigh(own[head], highest, seen_own, kv_own, head)
            earlier, total_earlier = weigh(prev[head], highest, seen_prev, kv_prev, head)
            attend(head, here + earlier, total_here + total_earlier)


    def partial_of(role, k):
        if k == 0:
            wout_loads[role].wait()
        return jnp.dot(att_v[...], wout_v[role, :, k * part : (k + 1) * part], preferred_element_type=jnp.float32)

    early = 2 * chunks - 1

    def sums_copy(slot, landing, device):
        return pltpu.make_async_remote_copy(
            src_ref=sums_s.at[slot], dst_ref=sums_r.at[landing],
            send_sem=sums_send.at[0 if slot < early else 1], recv_sem=sums_recv.at[landing],
            device_id={"head": device}, device_id_type=MESH,
        )

    def piece_copy(piece, landing, device):
        return pltpu.make_async_remote_copy(
            src_ref=enc_s.at[piece], dst_ref=enc_r.at[landing],
            send_sem=enc_send, recv_sem=enc_recv.at[landing],
            device_id={"head": device}, device_id_type=MESH,
        )

    def finish(k, out, encoded, squares):
        if k == 0:
            for i in range(4, 7):
                loads[i].wait()
        cols = slice(k * part, (k + 1) * part)
        attn_ref[:, cols] = out
        hidden = res_v[:, cols].astype(jnp.float32) + out.astype(jnp.float32)
        squares = squares + jnp.sum(hidden * hidden, axis=1, keepdims=True)
        scaled = (hidden * gain_v[cols][None]).astype(jnp.bfloat16)
        encoded = encoded + lax.dot_general(scaled, wenc_v[:, cols], nt, preferred_element_type=jnp.float32)
        return encoded, squares

    split = ROPE + (LANES - ROPE) // 2
    coarse_lanes = lax.broadcasted_iota(jnp.int32, (PIECE, LANES), 1) < split

    def pack(piece, encoded, squares):
        coarse = squares.astype(jnp.bfloat16).astype(jnp.float32)
        sums = jnp.where(
            coarse_lanes,
            jnp.broadcast_to(coarse, (PIECE, LANES)), jnp.broadcast_to(squares - coarse, (PIECE, LANES)),
        )
        enc_s[piece, :, KVL:] = sums.astype(jnp.bfloat16)
        enc_s[piece, :, : KVL + ROPE] = encoded.astype(jnp.bfloat16)

    def unpack(packed):
        squares = packed[:, KVL + ROPE : KVL + ROPE + 1] + packed[:, KVL + split : KVL + split + 1]
        return packed[:, : KVL + ROPE], squares

    def sent(buffer, sem):
        pltpu.make_async_copy(buffer, buffer, sem).wait()

    def give_turn():
        @pl.when(r + 1 < n_rep)
        def _():
            sent(sums_s.at[:early], sums_send.at[0])
            pl.semaphore_signal(turn, inc=1, device_id={"rep": r + 1}, device_id_type=MESH)

    def await_turn():
        @pl.when(r >= 1)
        def _():
            pl.semaphore_wait(turn, 1)

    def conclude(near_half):
        for piece in range(pieces):
            if near_half is None:
                piece_copy(piece, piece, partner).wait_recv()
            piece_copy(piece, pieces + piece, other).wait_recv()
            near = (enc_r[piece] if near_half is None else near_half[piece]).astype(jnp.float32)
            whole, square_sum = unpack(near + enc_r[pieces + piece].astype(jnp.float32))
            scale = lax.rsqrt(square_sum / (width * n_head) + epsilon)
            next_ref[piece * PIECE : (piece + 1) * PIECE, :] = (whole * scale).astype(jnp.bfloat16)

    nothing = jnp.zeros((rows, KVL + ROPE), jnp.float32), jnp.zeros((rows, 1), jnp.float32)

    @pl.when(at_end)
    def _():
        for slot in range(3 * chunks):
            role, k = divmod(slot, chunks)
            if slot == chunks + 3:
                await_turn()
            sums_s[slot] = partial_of(role, k).astype(jnp.bfloat16)
            sums_copy(slot, slot, partner).start()
        give_turn()
        encoded, squares = nothing
        for k in range(chunks):
            mine = partial_of(3, k)
            sums_copy(k, k, partner).wait_recv()
            mine = mine + sums_r[k].astype(jnp.float32)
            sums_copy(k, chunks + k, partner).wait_recv()
            out = (mine + sums_r[chunks + k].astype(jnp.float32)).astype(jnp.bfloat16)
            encoded, squares = finish(k, out, encoded, squares)
        for piece in range(pieces):
            own_rows = slice(piece * PIECE, (piece + 1) * PIECE)
            pack(piece, encoded[own_rows], squares[own_rows])
            piece_copy(piece, piece, partner).start()
        conclude(None)

    @pl.when(at_mate)
    def _():
        for k in range(chunks):
            sums_s[2 * chunks + k] = partial_of(2, k).astype(jnp.bfloat16)
            sums_copy(2 * chunks + k, k, partner).start()
        pl.semaphore_wait(far_in, 1)
        for slot in range(2 * chunks):
            role, k = divmod(slot, chunks)
            mine = partial_of(role, k)
            sums_copy(slot, slot, partner).wait_recv()
            sums_s[slot] = (mine + sums_r[slot].astype(jnp.float32)).astype(jnp.bfloat16)
            if role == 0:
                sums_copy(slot, chunks + k, far_end).start()
            else:
                sums_copy(slot, 3 * chunks + k, other).start()
        encoded, squares = nothing
        for k in range(chunks):
            mine = partial_of(3, k)
            sums_copy(k, 3 * chunks + k, other).wait_recv()
            mine = mine + sums_r[3 * chunks + k].astype(jnp.float32)
            sums_copy(k, 2 * chunks + k, partner).wait_recv()
            out = (mine + sums_r[2 * chunks + k].astype(jnp.float32)).astype(jnp.bfloat16)
            encoded, squares = finish(k, out, encoded, squares)
        for piece in range(pieces):
            own_rows = slice(piece * PIECE, (piece + 1) * PIECE)
            piece_copy(piece, piece, partner).wait_recv()
            theirs, their_squares = unpack(enc_r[piece].astype(jnp.float32))
            pack(piece, encoded[own_rows] + theirs, squares[own_rows] + their_squares)
            piece_copy(piece, pieces + piece, far_end).start()
            piece_copy(piece, piece, partner).start()
        for piece in range(pieces):
            piece_copy(piece, pieces + piece, other).start()
        conclude(enc_s)

    for step in range(1, back + 1):
        @pl.when(c + step < n_ctx)
        def _():
            latent_copy(step).wait_send()
    @pl.when(at_mate | (r + 1 == n_rep))
    def _():
        sent(sums_s.at[:early], sums_send.at[0])

    sent(sums_s.at[early:], sums_send.at[1])
    all_pieces = pltpu.make_async_copy(enc_s, enc_s, enc_send)

    @pl.when(at_end)
    def _():
        all_pieces.wait()

    @pl.when(at_mate)
    def _():
        for _ in range(3):
            all_pieces.wait()


def write_out(attn_v, next_v, attn_hbm, next_hbm, sem):
    copies = [
        pltpu.make_async_copy(attn_v, attn_hbm, sem.at[0]),
        pltpu.make_async_copy(next_v, next_hbm, sem.at[1]),
    ]
    for copy in copies:
        copy.start()
    for copy in copies:
        copy.wait()


def fused(n_ctx, n_head, n_rep, queries, kv_latent, doc_ids, w_kv, w_out, w_enc, residual, norm_gain):
    rows = queries.shape[0]
    heads = w_kv.shape[1] // (NOPE + VDIM)
    width = residual.shape[1]
    part = width // CHUNKS
    pieces = rows // PIECE
    back = min(n_ctx - 1, -(-(n_ctx * rows // 2 - 1) // rows))
    bf16, f32 = jnp.bfloat16, jnp.float32
    hbm = pl.BlockSpec(memory_space=pltpu.HBM)
    vmem = pl.BlockSpec(memory_space=pltpu.VMEM)
    dma = pltpu.SemaphoreType.DMA
    done = pl.pallas_call(
        functools.partial(kernel, n_ctx, n_head, n_rep, back, CHUNKS),
        out_shape=(pltpu.VMEM((rows, width), bf16), pltpu.VMEM((rows, KVL + ROPE), bf16)),
        in_specs=[hbm] * 8,
        out_specs=(vmem, vmem),
        scratch_shapes=[
            pltpu.VMEM(queries.shape, bf16),
            pltpu.VMEM(kv_latent.shape, bf16),
            pltpu.VMEM((1, rows), jnp.int32),
            pltpu.VMEM(w_kv.shape, bf16),
            pltpu.VMEM((4, w_out.shape[0], width), bf16),
            pltpu.VMEM(w_enc.shape[::-1], bf16),
            pltpu.VMEM(residual.shape, bf16),
            pltpu.VMEM((width,), f32),
            pltpu.VMEM((back + 1, rows, KVL + LANES), bf16),
            pltpu.VMEM((rows, heads * VDIM), bf16),
            pltpu.VMEM((3 * CHUNKS, rows, part), bf16),
            pltpu.VMEM((4 * CHUNKS, rows, part), bf16),
            pltpu.VMEM((pieces, PIECE, KVL + LANES), bf16),
            pltpu.VMEM((2 * pieces, PIECE, KVL + LANES), bf16),
            dma((7,)),
            dma((4,)),
            dma((back,)),
            dma((back,)),
            dma((2,)),
            dma((4 * CHUNKS,)),
            dma,
            dma((2 * pieces,)),
            pltpu.SemaphoreType.REGULAR,
            pltpu.SemaphoreType.REGULAR,
        ],
        compiler_params=pltpu.CompilerParams(
            collective_id=0, has_side_effects=True, vmem_limit_bytes=VMEM_BYTES
        ),
        name="latent_layer",
    )(
        queries, kv_latent, doc_ids[None], w_kv, w_out, w_enc.T, residual, norm_gain,
    )
    return pl.pallas_call(
        write_out,
        out_shape=tuple(pltpu.HBM(one.shape, one.dtype) for one in done),
        in_specs=[vmem] * 2,
        out_specs=(hbm, hbm),
        scratch_shapes=[dma((2,))],
        name="write_out",
    )(*[pltpu.with_memory_space_constraint(one, pltpu.VMEM) for one in done])


def general(n_ctx, n_head, n_rep, queries, kv_latent, doc_ids, w_kv, w_out, w_enc, residual, norm_gain):
    rows_here = queries.shape[0]
    heads_here = w_kv.shape[1] // (NOPE + VDIM)
    query_heads = queries.reshape(rows_here, heads_here, NOPE + ROPE)
    q_nope = query_heads[:, :, :NOPE]
    q_rope = query_heads[:, :, NOPE:]
    positions = lax.axis_index("ctx") * rows_here + lax.iota(jnp.int32, rows_here)
    weights = w_kv.reshape(KVL, heads_here, NOPE + VDIM)
    f32 = jnp.float32
    latents = lax.all_gather(kv_latent, "ctx", axis=0, tiled=True)
    key_docs = lax.all_gather(doc_ids, "ctx", axis=0, tiled=True)
    key_pos = lax.iota(jnp.int32, latents.shape[0])
    content = latents[:, :KVL]
    rotary = latents[:, KVL:]
    both = jnp.einsum("nc,chd->nhd", content, weights, preferred_element_type=f32).astype(jnp.bfloat16)
    keys = both[:, :, :NOPE]
    values = both[:, :, NOPE:]
    scores = jnp.einsum("qhd,nhd->hqn", q_nope, keys, preferred_element_type=f32)
    scores = scores + jnp.einsum("qhd,nd->hqn", q_rope, rotary, preferred_element_type=f32)
    visible = (key_docs[None, :] == doc_ids[:, None]) & (key_pos[None, :] <= positions[:, None])
    scores = jnp.where(visible[None], scores * (1.0 / math.sqrt(NOPE + ROPE)), masked_score)
    highest = jnp.max(scores, axis=2)
    probs = jnp.where(visible[None], jnp.exp(scores - highest[:, :, None]), 0.0)
    total = jnp.sum(probs, axis=2)
    mixed = jnp.einsum("hqn,nhd->hqd", probs.astype(jnp.bfloat16), values, preferred_element_type=f32)
    attended = (mixed / total[:, :, None]).astype(jnp.bfloat16)
    side_by_side = attended.transpose(1, 0, 2).reshape(rows_here, heads_here * VDIM)
    summed = lax.psum_scatter(
        lax.dot_general(w_out, side_by_side, (((0,), (1,)), ((), ())), preferred_element_type=f32),
        "head", scatter_dimension=0, tiled=True,
    )
    attn_out = summed.T.astype(jnp.bfloat16)
    hidden = residual.astype(f32) + attn_out.astype(f32)
    squares = jnp.sum(hidden * hidden, axis=1)
    scaled = (hidden * norm_gain[None, :]).astype(jnp.bfloat16)
    encoded = jnp.dot(scaled, w_enc, preferred_element_type=f32)
    enc_sum, sq_sum = lax.psum((encoded, squares), "head")
    next_latent = (enc_sum * lax.rsqrt(sq_sum / D + epsilon)[:, None]).astype(jnp.bfloat16)
    return (attn_out, next_latent)


def per_device(n_ctx, n_head, n_rep, *args):
    rows, width = args[6].shape
    whole_tiles = width % (CHUNKS * LANES) == 0 and rows % PIECE == 0 and rows <= LANES
    line = n_head == 4 and n_rep == 2
    body = fused if line and whole_tiles else general
    return body(n_ctx, n_head, n_rep, *args)


def solution(mesh):
    return jax.shard_map(
        functools.partial(per_device, mesh.shape["ctx"], mesh.shape["head"], mesh.shape["rep"]),
        mesh=mesh,
        in_specs=(
            P(("rep", "ctx"), "head"),
            P(("rep", "ctx"), None),
            P(("rep", "ctx")),
            P(None, "head"),
            P("head", None),
            P("head", None),
            P(("rep", "ctx"), "head"),
            P("head"),
        ),
        out_specs=(P(("rep", "ctx"), "head"), P(("rep", "ctx"), None)),
        check_vma=False,
    )
```
